32 devices in a mesh: dp: 16 (over z, y, core), tensor: 2 (over x).
Axes of the slice: x: 2, y: 2, z: 4, core: 2. Of those that a mesh axis runs over, the one named last changes fastest.
Arguments:
- activations: bfloat16 [32768, 1024], P(('dp', 'tensor')), may hold values from -6 to 6
- gradients: bfloat16 [32768, 5472], P('dp', 'tensor'), may hold values from -6 to 6
- act_history: float32 [2, 16, 1024], P('tensor'), may hold values from 0.1 to 4
- grad_history: float32 [16, 5472], P(None, 'tensor'), may hold values from 0.1 to 4
- owner_rank: int32 [1024], replicated, may hold values from 0 to 1
- history_slot: int32 [6496], replicated, may hold values from 0 to 15
Outputs:
- weight_grad: float32 [1024, 5472], P('dp', 'tensor')
- act_history_out: float32 [2, 16, 1024], P('tensor')
- grad_history_out: float32 [16, 5472], P(None, 'tensor')
The draws below stay inside these ranges and needn't reach their ends.
All inputs are finite; a program needn't handle non-finite values.
Results may differ from the reference program's by a relative error of at most 0.0042.
Values may be sent and summed in bfloat16 or wider, within the bound.
A program may use at most 64 MiB of HBM per device.

```python
import math
import jax
import jax.numpy as jnp
from jax import lax

D = 1024
FF = 5472
HIST = 16
TOKENS = 32768
N_TENSOR = 2


def set_ends(values, own_key, least, high):
    longest = values.shape.index(max(values.shape))
    spots = []
    for shift in (0, 1):
        where = [jax.random.randint(jax.random.fold_in(own_key, axis), (), 0, length) for axis, length in enumerate(values.shape)]
        where[longest] = (where[longest] + shift) % values.shape[longest]
        spots.append(tuple(where))
    return values.at[spots[0]].set(least).at[spots[1]].set(high)


def with_spikes(values, own_key, source, target, shards_of, factor):
    owner, partner = [(jnp.arange(values.shape[dim]) // (values.shape[dim] // shards_of)).reshape([-1 if axis == dim else 1 for axis in range(values.ndim)]) for dim in (source, target)]
    chosen = jax.random.permutation(own_key, shards_of)[partner]
    strong = (owner == chosen) | (owner == (partner + shards_of // 2) % shards_of)
    return jnp.where(strong, factor * values, values)


def shard_levels(stream_key, shape, cuts, least, largest):
    def one(position, shards_of):
        draws = jax.random.uniform(jax.random.fold_in(jax.random.fold_in(stream_key, 6), position), (shards_of,), jnp.float32, least / len(cuts), largest / len(cuts))
        return jnp.repeat(jnp.exp(draws), shape[position] // shards_of).reshape((-1,) + (1,) * (len(shape) - position - 1))

    factor_of = one(*cuts[0])
    for cut in cuts[1:]:
        factor_of = factor_of * one(*cut)
    return factor_of


def gaussian(key, shape, width, limit, split=(), held_as=jnp.bfloat16):
    result = jax.random.normal(key, shape, jnp.float32) * width
    if len(split) > 0:
        result = shard_levels(key, shape, split, -0.22, 0.18) * result
    return jnp.clip(result, min=-limit, max=limit).astype(held_as)


def bell_draw_with(own_key, shape, deviation, most, split, heavy, held_as=jnp.bfloat16):
    result = deviation * jax.random.normal(own_key, shape, jnp.float32)
    if split:
        result = result * shard_levels(own_key, shape, split, -0.22, 0.18)
    return jnp.clip(with_spikes(result, jax.random.fold_in(own_key, 3), *heavy), -most, most).astype(held_as)


def setup_inputs(seed: int = 0) -> dict:
    splits = jax.random.split(jax.random.key(seed), 7)
    return {
        "activations": bell_draw_with(splits[0], (TOKENS, D), 1.0, 6.0, ((0, 32),), (0, 1, 32, 2.75)),
        "gradients": gaussian(splits[1], (TOKENS, FF), 1.0, 6.0, ((0, 16), (1, 2))),
        "act_history": jnp.clip(jnp.exp(math.log(4.0) - 3.6888794 * jax.random.uniform(splits[2], (N_TENSOR, HIST, D), jnp.float32) ** shard_levels(splits[2], (N_TENSOR, HIST, D), ((0, 2),), -0.2, 0.2)), 0.1, 4.0),
        "grad_history": jnp.clip(jnp.exp(math.log(4.0) - 3.6888794 * jax.random.uniform(splits[3], (HIST, FF), jnp.float32) ** shard_levels(splits[3], (HIST, FF), ((1, 2),), -0.2, 0.2)), 0.1, 4.0),
        "owner_rank": set_ends(jax.random.randint(splits[4], (D,), 0, N_TENSOR), jax.random.fold_in(splits[4], 1), 0, N_TENSOR - 1).astype(jnp.int32),
        "history_slot": set_ends(jax.random.randint(splits[5], (D + FF,), 0, HIST), jax.random.fold_in(splits[5], 1), 0, HIST - 1).astype(jnp.int32),
    }


QUANT_LIMIT = 448.0
SCALE_FLOOR = 0.25

def quantize(values, scale):
    scaled = values.astype(jnp.float32) * scale
    return jnp.clip(scaled, -QUANT_LIMIT, QUANT_LIMIT).astype(jnp.bfloat16)

def place_peaks(history, peaks, slots):
    rows = lax.broadcasted_iota(jnp.int32, history.shape, 0)
    return jnp.where(rows == slots.astype(jnp.int32)[None, :], peaks[None, :], history)

def reference(activations, gradients, act_history, grad_history, owner_rank, history_slot):
    ranks = lax.broadcasted_iota(jnp.int32, act_history.shape, 0)
    picked = jnp.where(ranks == owner_rank.astype(jnp.int32)[None, None, :], act_history, jnp.float32(0.0))
    current_history = lax.optimization_barrier(jnp.sum(picked, axis=0))
    act_scale = QUANT_LIMIT / jnp.maximum(lax.optimization_barrier(jnp.max(current_history, axis=0)), SCALE_FLOOR)
    grad_scale = QUANT_LIMIT / jnp.maximum(lax.optimization_barrier(jnp.max(grad_history, axis=0)), SCALE_FLOOR)
    act_quant = quantize(activations, act_scale)
    block_width = FF // 4
    results = []
    for block_index in range(4):
        first_col = block_index * block_width
        grad_block = quantize(gradients[:, first_col:first_col + block_width], grad_scale[first_col:first_col + block_width])
        results.append(jnp.dot(act_quant.T, grad_block, preferred_element_type=jnp.float32))
    summed = jnp.concatenate(results, axis=1)
    grad_factor = 1.0 / math.sqrt(TOKENS)
    weight_grad = summed / (act_scale[:, None] * grad_scale[None, :]) * grad_factor
    act_peak = lax.optimization_barrier(jnp.max(jnp.abs(activations), axis=0)).astype(jnp.float32)
    grad_peak = lax.optimization_barrier(jnp.max(jnp.abs(gradients), axis=0)).astype(jnp.float32)
    updated = place_peaks(current_history, act_peak, history_slot[:D])
    act_history_out = jnp.broadcast_to(updated[None], (N_TENSOR, HIST, D))
    grad_history_out = place_peaks(grad_history, grad_peak, history_slot[D:])
    return (weight_grad, act_history_out, grad_history_out)
```

```python
import functools
import math

import jax
import jax.numpy as jnp
from jax import lax
from jax.experimental import pallas as pl
from jax.experimental.pallas import tpu as pltpu
from jax.sharding import PartitionSpec as P

QUANT_LIMIT = 448.0
SCALE_FLOOR = 0.25
CORES = 2
ROWS_Y = 2
LANES = 128
SUBLANES = 16
PIECES = 2
OWN_TILE = 768
GOT_TILE = 1536
TURN = 256
MESH = pl.DeviceIdType.MESH


def quantize(values, scale):
    scaled = values.astype(jnp.float32) * scale
    return jnp.clip(scaled, -QUANT_LIMIT, QUANT_LIMIT).astype(jnp.bfloat16)


def place_peaks(history, peaks, slots):
    rows = lax.broadcasted_iota(jnp.int32, history.shape, 0)
    return jnp.where(rows == slots[None, :], peaks[None, :], history)


def tiles(width, step):
    return [(start, min(step, width - start)) for start in range(0, width, step)]


def fused_kernel(
    dp, tensor,
    act_hbm, grad_hbm, act_hist_hbm, grad_hist_hbm, owner_hbm, slot_hbm,
    weight_ref, act_hist_out, grad_hist_out,
    act_own, act_down, act_got, raw, gq, part, core_got, y_out, y_got, z_out, z_got,
    own_lhs, got_lhs, act_hist, hist_got, grad_hist, owner_ref, slot_ref,
    core_peaks, y_peaks, z_peaks, act_peaks,
    act_scale, scale_down, grad_scale, current_hist,
    load_sem, grad_sem, small_sem, hist_send, hist_recv, pair_send, pair_recv,
    x_send, x_recv, core_send, core_recv, y_send, y_recv, z_send, z_recv,
    pk_send, pk_recv, ap_send, ap_recv,
):
    me = lax.axis_index("dp")
    mt = lax.axis_index("tensor")
    core = lax.rem(me, CORES)
    chip = lax.div(me, CORES)
    yy = lax.rem(chip, ROWS_Y)
    zz = lax.div(chip, ROWS_Y)
    depth = dp // (CORES * ROWS_Y)
    tokens, width = act_hbm.shape
    cols, rows = grad_hbm.shape
    block = width // dp
    piece = block // PIECES
    padded = grad_scale.shape[1]
    full, rest = cols // LANES, cols % LANES
    own_tiles = tiles(padded, OWN_TILE)
    got_tiles = tiles(padded, GOT_TILE)
    steps = ROWS_Y * PIECES

    def dp_index(z, y, c):
        return (z * ROWS_Y + y) * CORES + c

    def on_tensor(t):
        return {"tensor": lax.rem(mt + t, tensor)}

    sibling = {"dp": dp_index(zz, yy, 1 - core)}
    y_peer = {"dp": dp_index(zz, 1 - yy, core)}

    def on_z(k):
        return {"dp": dp_index(lax.rem(zz + k, depth), yy, core)}

    barrier = pltpu.get_barrier_semaphore()
    partners = [on_tensor(t) for t in range(1, tensor)] + [sibling, y_peer]
    partners += [on_z(k) for k in range(1, depth)]
    for partner in partners:
        pl.semaphore_signal(barrier, inc=1, device_id=partner, device_id_type=MESH)

    act_load = pltpu.make_async_copy(act_hbm, act_own, load_sem)
    act_load.start()
    smalls = [
        pltpu.make_async_copy(source, target, small_sem.at[i])
        for i, (source, target) in enumerate((
            (grad_hist_hbm, grad_hist), (act_hist_hbm, act_hist),
            (owner_hbm, owner_ref), (slot_hbm, slot_ref),
        ))
    ]
    for small in smalls:
        small.start()

    def grad_load(i, size=LANES):
        at = pl.ds(i * LANES, size)
        return pltpu.make_async_copy(grad_hbm.at[at], raw.at[at], grad_sem.at[i])

    def start_load(i, carry):
        grad_load(i).start()
        return carry

    lax.fori_loop(0, full, start_load, 0)
    if rest:
        grad_load(full, rest).start()
        raw[cols:, :] = jnp.zeros((padded - cols, rows), jnp.bfloat16)

    def offset_z(u):
        if depth == 4:
            return 2 - u + 3 * lax.div(u, 2) + 2 * lax.div(u, 3)
        return u + 1

    def target_z(u):
        return lax.rem(zz + offset_z(u), depth)

    def side(k):
        return yy * k + (1 - yy) * (1 - k)

    def pair_at(u, k):
        return pl.ds((target_z(u) * ROWS_Y + side(k)) * CORES, CORES)

    def piece_at(s):
        return pl.ds(s * piece, piece)

    def part_rows(k, c, s):
        return pl.ds(
            pl.multiple_of((side(k) * CORES + c) * block + s * piece, piece), piece
        )

    def step_of(u, k, s):
        return u * steps + k * PIECES + s

    def hist_copy(t):
        at = pl.ds(pl.multiple_of(core * (width // CORES), LANES), width // CORES)
        return pltpu.make_async_remote_copy(
            src_ref=act_hist_hbm.at[0, :, at], dst_ref=hist_got.at[t - 1, :, at],
            send_sem=hist_send.at[t - 1], recv_sem=hist_recv.at[t - 1],
            device_id=on_tensor(t), device_id_type=MESH,
        )

    def hist_pass(t):
        at = pl.ds(pl.multiple_of(core * (width // CORES), LANES), width // CORES)
        return pltpu.make_async_remote_copy(
            src_ref=hist_got.at[t - 1, :, at], dst_ref=hist_got.at[t - 1, :, at],
            send_sem=pair_send.at[t - 1], recv_sem=pair_recv.at[t - 1],
            device_id=sibling, device_id_type=MESH,
        )

    def x_copy(t, u, k, s):
        at = step_of(u, k, s)
        return pltpu.make_async_remote_copy(
            src_ref=act_down.at[pair_at(u, k), piece_at(s)],
            dst_ref=act_got.at[t - 1, pair_at(u, k), piece_at(s)],
            send_sem=x_send.at[t - 1, at], recv_sem=x_recv.at[t - 1, at],
            device_id=on_tensor(t), device_id_type=MESH,
        )

    def core_copy(u, k, s, j):
        at = step_of(u, k, s)
        start, size = got_tiles[j]
        return pltpu.make_async_remote_copy(
            src_ref=part.at[u, part_rows(k, 1 - core, s), pl.ds(start, size)],
            dst_ref=core_got.at[at, :, pl.ds(start, size)],
            send_sem=core_send.at[at, j], recv_sem=core_recv.at[at, j],
            device_id=sibling, device_id_type=MESH,
        )

    def y_copy(u, s):
        return pltpu.make_async_remote_copy(
            src_ref=y_out.at[u, piece_at(s)], dst_ref=y_got.at[u, piece_at(s)],
            send_sem=y_send.at[u, s], recv_sem=y_recv.at[u, s],
            device_id=y_peer, device_id_type=MESH,
        )

    def z_copy(u, s):
        return pltpu.make_async_remote_copy(
            src_ref=z_out.at[u, piece_at(s)], dst_ref=z_got.at[u, piece_at(s)],
            send_sem=z_send.at[u, s], recv_sem=z_recv.at[u, s],
            device_id=on_z(offset_z(u)), device_id_type=MESH,
        )

    def peak_copy(buffer, i, partner, at):
        return pltpu.make_async_remote_copy(
            src_ref=buffer.at[0], dst_ref=buffer.at[i],
            send_sem=pk_send.at[at], recv_sem=pk_recv.at[at],
            device_id=partner, device_id_type=MESH,
        )

    core_peak = peak_copy(core_peaks, 1, sibling, 0)
    y_peak = peak_copy(y_peaks, 1, y_peer, 1)
    z_peak = [peak_copy(z_peaks, k, on_z(k), 1 + k) for k in range(1, depth)]

    def act_peak_copy(t):
        return pltpu.make_async_remote_copy(
            src_ref=act_peaks.at[0], dst_ref=act_peaks.at[t],
            send_sem=ap_send.at[t - 1], recv_sem=ap_recv.at[t - 1],
            device_id=on_tensor(t), device_id_type=MESH,
        )

    act_load.wait()

    def turn_act(b, carry):
        at = pl.ds(pl.multiple_of(b * LANES, LANES), LANES)
        read = act_own[:, at]
        top = jnp.max(jnp.abs(read).reshape(tokens // SUBLANES, SUBLANES, LANES), axis=0)
        core_peaks[0, :, at] = jnp.max(top.astype(jnp.float32), axis=0, keepdims=True)
        act_down[pl.ds(b * (LANES // block), LANES // block)] = jnp.transpose(read).reshape(
            LANES // block, block, tokens
        )
        return carry

    lax.fori_loop(0, width // LANES, turn_act, 0)

    pl.semaphore_wait(barrier, len(partners))
    for t in range(1, tensor):
        hist_copy(t).start()

    def send_x(u, carry):
        for k in range(ROWS_Y):
            for s in range(PIECES):
                for t in range(1, tensor):
                    x_copy(t, u, k, s).start()
        return carry

    lax.fori_loop(0, depth, send_x, 0)

    smalls[0].wait()
    if rest:
        grad_scale[:, padded - LANES:] = jnp.ones((1, LANES), jnp.float32)
    grad_scale[:, :cols] = QUANT_LIMIT / jnp.maximum(
        jnp.max(grad_hist[...], axis=0, keepdims=True), SCALE_FLOOR
    )

    def quantize_cols(j):
        at = pl.ds(pl.multiple_of(j * LANES, LANES), LANES)
        scale = grad_scale[:, at]
        top = jnp.zeros((SUBLANES, LANES), jnp.bfloat16)
        for start, size in tiles(rows, TURN):
            turned = jnp.transpose(raw[at, start:start + size])
            mag = jnp.abs(turned).reshape(size // SUBLANES, SUBLANES, LANES)
            top = jnp.maximum(top, jnp.max(mag, axis=0))
            gq[start:start + size, at] = quantize(turned, scale)
        here = pl.ds(pl.multiple_of(width + j * LANES, LANES), LANES)
        core_peaks[0, :, here] = jnp.max(top.astype(jnp.float32), axis=0, keepdims=True)

    def grad_chunk(i, carry):
        grad_load(i).wait()
        quantize_cols(i)
        return carry

    lax.fori_loop(0, full // 2, grad_chunk, 0)
    for t in range(1, tensor):
        hist_copy(t).wait()
        hist_pass(t).start()
    lax.fori_loop(full // 2, full, grad_chunk, 0)
    if rest:
        grad_load(full, rest).wait()
        quantize_cols(full)
    core_peak.start()

    for small in smalls[1:]:
        small.wait()
    owner = owner_ref[...]
    current = jnp.where(owner == mt, act_hist[0], 0.0)
    for t in range(1, tensor):
        hist_pass(t).wait()
        source = lax.rem(mt + tensor - t, tensor)
        current = jnp.where(owner == source, hist_got[t - 1], current)
    current_hist[...] = current
    act_scale[...] = QUANT_LIMIT / jnp.maximum(
        jnp.max(current, axis=0, keepdims=True), SCALE_FLOOR
    )
    for start in range(0, width, LANES):
        turned = jnp.transpose(jnp.broadcast_to(act_scale[:, start:start + LANES], (LANES, LANES)))
        first = start // block
        scale_down[first:first + LANES // block] = turned.reshape(LANES // block, block, LANES)

    def load_own(u):
        at = pl.ds(target_z(u) * (ROWS_Y * CORES), ROWS_Y * CORES)
        count = ROWS_Y * CORES * block
        scale = scale_down[at].reshape(count, LANES)
        for start in range(0, tokens, LANES):
            read = act_down[at, :, start:start + LANES].reshape(count, LANES)
            own_lhs[:, start:start + LANES] = quantize(read, scale)

    def own_product(u, j):
        start, size = own_tiles[j]
        source = pl.ds(pl.multiple_of(mt * tokens, tokens), tokens)
        part[u, :, start:start + size] = jnp.dot(
            own_lhs[...], gq[source, start:start + size], preferred_element_type=jnp.float32
        )

    def got_product(u, k, s):
        scale = scale_down[pair_at(u, k), piece_at(s), :].reshape(CORES * piece, LANES)
        for t in range(1, tensor):
            x_copy(t, u, k, s).wait_recv()
            for start in range(0, tokens, LANES):
                read = act_got[t - 1, pair_at(u, k), piece_at(s), start:start + LANES]
                got_lhs[t - 1, :, start:start + LANES] = quantize(
                    read.reshape(CORES * piece, LANES), scale
                )
        for j, (start, size) in enumerate(got_tiles):
            for t in range(1, tensor):
                from_rank = lax.rem(mt + tensor - t, tensor)
                source = pl.ds(pl.multiple_of(from_rank * tokens, tokens), tokens)
                term = jnp.dot(
                    got_lhs[t - 1], gq[source, start:start + size],
                    preferred_element_type=jnp.float32,
                )
                for c in range(CORES):
                    part[u, part_rows(k, c, s), start:start + size] += term[
                        c * piece:(c + 1) * piece
                    ]
            core_copy(u, k, s, j).start()

    def core_sum(u, k, s, j):
        start, size = got_tiles[j]
        core_copy(u, k, s, j).wait_recv()
        return (
            part[u, part_rows(k, core, s), start:start + size]
            + core_got[step_of(u, k, s), :, start:start + size]
        )

    def send_y(u, s):
        for j, (start, size) in enumerate(got_tiles):
            y_out[u, piece_at(s), start:start + size] = core_sum(u, 0, s, j).astype(jnp.bfloat16)
        y_copy(u, s).start()

    def line_sum(u, s, j):
        start, size = got_tiles[j]
        return core_sum(u, 1, s, j) + y_got[u, piece_at(s), start:start + size].astype(jnp.float32)

    def send_z(u, s):
        y_copy(u, s).wait_recv()
        for j, (start, size) in enumerate(got_tiles):
            z_out[u, piece_at(s), start:start + size] = line_sum(u, s, j).astype(jnp.bfloat16)
        z_copy(u, s).start()

    def unit(u):
        for k in range(ROWS_Y):
            for s in range(PIECES):
                got_product(u, k, s)
                if k == 0 and s == 0:
                    load_own(u + 1)
                for j in range(k * PIECES + s, len(own_tiles), steps):
                    own_product(u + 1, j)
                if k == 0:
                    send_y(u, s)
                else:
                    send_z(u, s)

    load_own(0)
    for j in range(len(own_tiles)):
        own_product(0, j)
    core_peak.wait()
    y_peaks[0] = jnp.max(core_peaks[...], axis=0)
    y_peak.start()

    unit(0)
    y_peak.wait()
    z_peaks[0] = jnp.max(y_peaks[...], axis=0)
    for copy in z_peak:
        copy.start()

    def middle(u, carry):
        unit(u)
        return carry

    lax.fori_loop(1, depth - 1, middle, 0)

    last = depth - 1
    got_product(last, 0, 0)
    for copy in z_peak:
        copy.wait()
    tops = jnp.max(z_peaks[...], axis=0)
    act_peaks[0] = tops[:, :width]
    for t in range(1, tensor):
        act_peak_copy(t).start()
    send_y(last, 0)
    for s in range(1, PIECES):
        got_product(last, 0, s)
        send_y(last, s)

    hist_row = lax.broadcasted_iota(jnp.int32, grad_hist.shape, 0)
    slots = slot_ref[...]
    grad_slots = slots[width:width + cols]
    for t in range(1, tensor):
        first = width + t * cols
        grad_slots = jnp.where(mt == t, slots[first:first + cols], grad_slots)
    grad_hist_out[...] = jnp.where(
        hist_row == grad_slots[None, :], tops[:, width:width + cols], grad_hist[...]
    )
    for t in range(1, tensor):
        act_peak_copy(t).wait()
    hist_row = lax.broadcasted_iota(jnp.int32, current_hist.shape, 0)
    act_hist_out[0] = jnp.where(
        hist_row == slots[:width][None, :], jnp.max(act_peaks[...], axis=0), current_hist[...]
    )
    factor = 1.0 / math.sqrt(rows * dp)
    grad_scale[...] = factor / grad_scale[...]
    undo = 1.0 / scale_down[me]

    for s in range(PIECES):
        got_product(last, 1, s)
        y_copy(last, s).wait_recv()
        for u in range(depth - 1):
            z_copy(u, s).wait_recv()
        for j, (start, size) in enumerate(got_tiles):
            total = line_sum(last, s, j)
            for u in range(depth - 1):
                total = total + z_got[u, piece_at(s), start:start + size].astype(jnp.float32)
            total = total * undo[s * piece:(s + 1) * piece, :1]
            total = total * grad_scale[:, start:start + size]
            size = min(size, cols - start)
            weight_ref[piece_at(s), start:start + size] = total[:, :size]

    def finish(u, carry):
        for s in range(PIECES):
            for k in range(ROWS_Y):
                for t in range(1, tensor):
                    x_copy(t, u, k, s).wait_send()
                for j in range(len(got_tiles)):
                    core_copy(u, k, s, j).wait_send()
            y_copy(u, s).wait_send()
        return carry

    lax.fori_loop(0, depth, finish, 0)

    def finish_z(u, carry):
        for s in range(PIECES):
            z_copy(u, s).wait_send()
        return carry

    lax.fori_loop(0, depth - 1, finish_z, 0)


def fused_outputs(activations, gradients, act_history, grad_history, owner_rank, history_slot):
    dp, tensor = lax.axis_size("dp"), lax.axis_size("tensor")
    tokens, width = activations.shape
    rows, cols = gradients.shape
    hist = act_history.shape[1]
    depth = dp // (CORES * ROWS_Y)
    blocks, block = dp, width // dp
    steps = depth * ROWS_Y * PIECES
    padded = pl.cdiv(cols, LANES) * LANES
    line = ROWS_Y * CORES * block
    dma = pltpu.SemaphoreType.DMA
    vmem = pl.BlockSpec(memory_space=pltpu.VMEM)
    hbm = pl.BlockSpec(memory_space=pl.ANY)
    f32, bf16, i32 = jnp.float32, jnp.bfloat16, jnp.int32
    others = tensor - 1
    halves = len(tiles(padded, GOT_TILE))
    return pl.pallas_call(
        functools.partial(fused_kernel, dp, tensor),
        out_shape=(
            pltpu.VMEM((block, cols), f32),
            pltpu.VMEM((1, hist, width), f32),
            pltpu.VMEM((hist, cols), f32),
        ),
        in_specs=[hbm] * 6,
        out_specs=(vmem, vmem, vmem),
        scratch_shapes=[
            pltpu.VMEM((tokens, width), bf16),
            pltpu.VMEM((blocks, block, tokens), bf16),
            pltpu.VMEM((others, blocks, block, tokens), bf16),
            pltpu.VMEM((padded, rows), bf16),
            pltpu.VMEM((rows, padded), bf16),
            pltpu.VMEM((depth, line, padded), f32),
            pltpu.VMEM((steps, block // PIECES, padded), f32),
            pltpu.VMEM((depth, block, padded), bf16),
            pltpu.VMEM((depth, block, padded), bf16),
            pltpu.VMEM((depth - 1, block, padded), bf16),
            pltpu.VMEM((depth - 1, block, padded), bf16),
            pltpu.VMEM((line, tokens), bf16),
            pltpu.VMEM((others, CORES * (block // PIECES), tokens), bf16),
            pltpu.VMEM((1, hist, width), f32),
            pltpu.VMEM((others, hist, width), f32),
            pltpu.VMEM((hist, cols), f32),
            pltpu.VMEM((1, width), i32),
            pltpu.VMEM(history_slot.shape, i32),
            pltpu.VMEM((2, 1, width + padded), f32),
            pltpu.VMEM((2, 1, width + padded), f32),
            pltpu.VMEM((depth, 1, width + padded), f32),
            pltpu.VMEM((tensor, 1, width), f32),
            pltpu.VMEM((1, width), f32),
            pltpu.VMEM((blocks, block, LANES), f32),
            pltpu.VMEM((1, padded), f32),
            pltpu.VMEM((hist, width), f32),
            dma, dma((padded // LANES,)), dma((4,)), dma((others,)), dma((others,)),
            dma((others,)), dma((others,)),
            dma((others, steps)), dma((others, steps)), dma((steps, halves)), dma((steps, halves)),
            dma((depth, PIECES)), dma((depth, PIECES)), dma((depth - 1, PIECES)), dma((depth - 1, PIECES)),
            dma((depth + 1,)), dma((depth + 1,)), dma((others,)), dma((others,)),
        ],
        compiler_params=pltpu.CompilerParams(
            collective_id=0, has_side_effects=True, vmem_limit_bytes=61 * 1024 * 1024
        ),
    )(
        activations, gradients.T, act_history, grad_history,
        owner_rank[None, :], history_slot,
    )


def hand_over_kernel(*refs):
    sems = refs[-1]
    half = (len(refs) - 1) // 2
    copies = [
        pltpu.make_async_copy(source, target, sems.at[i])
        for i, (source, target) in enumerate(zip(refs[:half], refs[half:-1]))
    ]
    for copy in copies:
        copy.start()
    for copy in copies:
        copy.wait()


def hand_over(*results):
    vmem = pl.BlockSpec(memory_space=pltpu.VMEM)
    hbm = pl.BlockSpec(memory_space=pl.ANY)
    return pl.pallas_call(
        hand_over_kernel,
        out_shape=tuple(jax.ShapeDtypeStruct(r.shape, r.dtype) for r in results),
        in_specs=[vmem] * len(results),
        out_specs=(hbm,) * len(results),
        scratch_shapes=[pltpu.SemaphoreType.DMA((len(results),))],
        compiler_params=pltpu.CompilerParams(vmem_limit_bytes=1024 * 1024),
    )(*results)


def gathered_sums(activations, gradients, act_history, grad_history, owner_rank):
    my_rank = lax.axis_index("tensor")
    held = jnp.where(owner_rank[None, :] == my_rank, act_history[0], jnp.float32(0.0))
    current = lax.psum(held, "tensor")
    act_scale = QUANT_LIMIT / jnp.maximum(jnp.max(current, axis=0), SCALE_FLOOR)
    grad_scale = QUANT_LIMIT / jnp.maximum(jnp.max(grad_history, axis=0), SCALE_FLOOR)
    gathered_rows = lax.all_gather(quantize(activations, act_scale), "tensor", axis=0, tiled=True)
    summed = lax.psum_scatter(
        lax.dot_general(
            gathered_rows, quantize(gradients, grad_scale), (((0,), (0,)), ((), ())),
            preferred_element_type=jnp.float32,
        ),
        "dp", scatter_dimension=0, tiled=True,
    )
    act_peak = lax.pmax(jnp.max(jnp.abs(activations), axis=0).astype(jnp.float32), ("dp", "tensor"))
    grad_peak = lax.pmax(jnp.max(jnp.abs(gradients), axis=0).astype(jnp.float32), "dp")
    return summed, current, act_peak[None, :], grad_peak[None, :]


def body(activations, gradients, act_history, grad_history, owner_rank, history_slot):
    dp = lax.axis_size("dp")
    model_width = act_history.shape[2]
    column_total = gradients.shape[1]
    row_count = model_width // dp
    fits = dp % (CORES * ROWS_Y) == 0 and dp > CORES * ROWS_Y
    fits = fits and LANES % row_count == 0 and row_count % (PIECES * SUBLANES) == 0
    fits = fits and model_width % (CORES * LANES) == 0 and activations.shape[0] % TURN == 0
    fits = fits and column_total % SUBLANES == 0
    if fits:
        return hand_over(*fused_outputs(
            activations, gradients, act_history, grad_history, owner_rank, history_slot
        ))
    act_slots = history_slot[:model_width]
    grad_slots = lax.dynamic_slice_in_dim(
        history_slot, model_width + lax.axis_index("tensor") * column_total, column_total, 0
    )
    summed, current, act_peak, grad_peak = gathered_sums(
        activations, gradients, act_history, grad_history, owner_rank
    )
    act_scale = QUANT_LIMIT / jnp.maximum(jnp.max(current, axis=0), SCALE_FLOOR)
    grad_scale = QUANT_LIMIT / jnp.maximum(jnp.max(grad_history, axis=0), SCALE_FLOOR)
    grad_factor = 1.0 / math.sqrt(gradients.shape[0] * dp)
    row_base = lax.axis_index("dp") * row_count
    row_scale = lax.dynamic_slice_in_dim(act_scale, row_base, row_count, 0)
    weight_grad = summed / (row_scale[:, None] * grad_scale[None, :]) * grad_factor
    act_history_out = place_peaks(current, act_peak[0], act_slots)[None]
    grad_history_out = place_peaks(grad_history, grad_peak[0], grad_slots)
    return (weight_grad, act_history_out, grad_history_out)


def solution(mesh):
    placed = (
        P(("dp", "tensor"), None),
        P("dp", "tensor"),
        P("tensor", None, None),
        P(None, "tensor"),
        P(),
        P(),
    )
    return jax.shard_map(
        body,
        mesh=mesh,
        in_specs=placed,
        out_specs=(P("dp", "tensor"), P("tensor", None, None), P(None, "tensor")),
        check_vma=False,
    )
```

```python
import functools
import math

import jax
import jax.numpy as jnp
from jax import lax
from jax.experimental import pallas as pl
from jax.experimental.pallas import tpu as pltpu
from jax.sharding import PartitionSpec as P

QUANT_LIMIT = 448.0
SCALE_FLOOR = 0.25
CORES = 2
ROWS_Y = 2
DEPTH = 4
LANES = 128
SUBLANES = 16
PIECES = 2
OWN_TILE = 768
GOT_TILE = 1536
TAIL_CUTS = 2
TURN = 256
MESH = pl.DeviceIdType.MESH


def quantize(values, scale):
    scaled = values.astype(jnp.float32) * scale
    return jnp.clip(scaled, -QUANT_LIMIT, QUANT_LIMIT).astype(jnp.bfloat16)


def place_peaks(history, peaks, slots):
    rows = lax.broadcasted_iota(jnp.int32, history.shape, 0)
    return jnp.where(rows == slots[None, :], peaks[None, :], history)


def tiles(width, step):
    return [(start, min(step, width - start)) for start in range(0, width, step)]


def fused_kernel(
    dp, tensor,
    act_hbm, grad_hbm, act_hist_hbm, grad_hist_hbm, owner_hbm, slot_hbm,
    weight_ref, act_hist_out, grad_hist_out,
    act_own, act_down, act_got, raw, gq, part, core_got, y_out, y_got, z_out, z_got,
    own_lhs, got_lhs, act_hist, hist_got, grad_hist, owner_ref, slot_ref,
    core_peaks, y_peaks, near_peaks, far_peaks, act_peaks,
    act_tops, act_scale, scale_down, grad_scale, grad_undo, far_sem,
    load_sem, grad_sem, small_sem, hist_send, hist_recv, top_send, top_recv,
    x_send, x_recv, core_send, core_recv, y_send, y_recv, z_send, z_recv,
    pk_send, pk_recv, ap_send, ap_recv,
):
    me = lax.axis_index("dp")
    mt = lax.axis_index("tensor")
    core = lax.rem(me, CORES)
    chip = lax.div(me, CORES)
    yy = lax.rem(chip, ROWS_Y)
    zz = lax.div(chip, ROWS_Y)
    depth = DEPTH
    half, odd = lax.div(zz, 2), lax.rem(zz, 2)
    inner = odd * (1 - half) + (1 - odd) * half
    beside = 2 * half + 1 - odd
    tokens, width = act_hbm.shape
    cols, rows = grad_hbm.shape
    block = width // dp
    piece = block // PIECES
    padded = grad_scale.shape[1]
    full, rest = cols // LANES, cols % LANES
    own_tiles = tiles(padded, OWN_TILE)
    got_tiles = tiles(padded, GOT_TILE)
    steps = ROWS_Y * PIECES
    last = depth - 1
    order = [(u, k, s) for u in range(depth) for k in range(ROWS_Y) for s in range(PIECES)]
    at = order.index((last, 0, 0))
    order[at - 1:at + 1] = [order[at], order[at - 1]]

    def dp_index(z, y, c):
        return (z * ROWS_Y + y) * CORES + c

    def on_tensor(t):
        return {"tensor": lax.rem(mt + t, tensor)}

    sibling = {"dp": dp_index(zz, yy, 1 - core)}
    y_peer = {"dp": dp_index(zz, 1 - yy, core)}

    def on_z(z):
        return {"dp": dp_index(z, yy, core)}

    z_near, z_far = on_z(beside), on_z(2 * (1 - half) + odd)

    barrier = pltpu.get_barrier_semaphore()
    partners = [on_tensor(t) for t in range(1, tensor)] + [sibling, y_peer]
    below = lax.div(zz + depth - 1, depth)
    above = 1 - lax.div(zz + 1, depth)

    def greet(semaphore):
        @pl.when(zz > 0)
        def _():
            pl.semaphore_signal(semaphore, inc=1, device_id=on_z(zz - 1), device_id_type=MESH)

        @pl.when(zz < depth - 1)
        def _():
            pl.semaphore_signal(semaphore, inc=1, device_id=on_z(zz + 1), device_id_type=MESH)

    for partner in partners:
        pl.semaphore_signal(barrier, inc=1, device_id=partner, device_id_type=MESH)
    greet(barrier)

    def target_z(u):
        return (3 * (1 - half), 2 - half, beside, zz)[u]

    def side(k):
        return yy * k + (1 - yy) * (1 - k)

    def pair_of(u, k):
        return target_z(u) * ROWS_Y + side(k)

    def pair_at(u, k):
        return pl.ds(pair_of(u, k) * CORES, CORES)

    def pair_cols(u, k):
        return pl.ds(pl.multiple_of(pair_of(u, k) * (CORES * block), LANES), CORES * block)

    def act_load(u, k):
        at = pair_cols(u, k)
        return pltpu.make_async_copy(
            act_hbm.at[:, at], act_own.at[:, at], load_sem.at[u * ROWS_Y + k]
        )

    for u in range(depth):
        for k in range(ROWS_Y):
            act_load(u, k).start()
    smalls = [
        pltpu.make_async_copy(source, target, small_sem.at[i])
        for i, (source, target) in enumerate((
            (grad_hist_hbm, grad_hist), (act_hist_hbm, act_hist),
            (owner_hbm, owner_ref), (slot_hbm, slot_ref),
        ))
    ]
    for small in smalls:
        small.start()

    def grad_load(i, size=LANES):
        at = pl.ds(i * LANES, size)
        return pltpu.make_async_copy(grad_hbm.at[at], raw.at[at], grad_sem.at[i])

    def start_load(i, carry):
        grad_load(i).start()
        return carry

    lax.fori_loop(0, full, start_load, 0)
    if rest:
        grad_load(full, rest).start()
        raw[cols:, :] = jnp.zeros((padded - cols, rows), jnp.bfloat16)

    def piece_at(s):
        return pl.ds(s * piece, piece)

    def part_rows(k, c, s):
        return pl.ds(
            pl.multiple_of((side(k) * CORES + c) * block + s * piece, piece), piece
        )

    def step_of(u, k, s):
        return u * steps + k * PIECES + s

    def hist_copy(t, stage):
        parts = CORES if stage == 2 else CORES * ROWS_Y
        mine = core if stage == 2 else core * ROWS_Y + yy
        at = pl.ds(pl.multiple_of(mine * (width // parts), LANES), width // parts)
        held = hist_got.at[t - 1, :, at]
        return pltpu.make_async_remote_copy(
            src_ref=held if stage else act_hist_hbm.at[0, :, at], dst_ref=held,
            send_sem=hist_send.at[t - 1, stage], recv_sem=hist_recv.at[t - 1, stage],
            device_id=(on_tensor(t), y_peer, sibling)[stage], device_id_type=MESH,
        )

    def top_copy(t):
        return pltpu.make_async_remote_copy(
            src_ref=act_tops.at[0], dst_ref=act_tops.at[t],
            send_sem=top_send.at[t - 1], recv_sem=top_recv.at[t - 1],
            device_id=on_tensor(t), device_id_type=MESH,
        )

    def pass_hist(stage):
        for t in range(1, tensor):
            hist_copy(t, stage - 1).wait()
            if stage < 3:
                hist_copy(t, stage).start()

    def x_copy(t, u, k, s, cut=0, cuts=1):
        at = step_of(u, k, s) + cut
        span = pl.ds(cut * (tokens // cuts), tokens // cuts)
        return pltpu.make_async_remote_copy(
            src_ref=act_down.at[pair_at(u, k), piece_at(s), span],
            dst_ref=act_got.at[t - 1, pair_at(u, k), piece_at(s), span],
            send_sem=x_send.at[t - 1, at], recv_sem=x_recv.at[t - 1, at],
            device_id=on_tensor(t), device_id_type=MESH,
        )

    def core_copy(u, k, s, j):
        at = step_of(u, k, s)
        start, size = got_tiles[j]
        return pltpu.make_async_remote_copy(
            src_ref=part.at[u, part_rows(k, 1 - core, s), pl.ds(start, size)],
            dst_ref=core_got.at[at, :, pl.ds(start, size)],
            send_sem=core_send.at[at, j], recv_sem=core_recv.at[at, j],
            device_id=sibling, device_id_type=MESH,
        )

    def y_copy(u, s, j):
        at = pl.ds(*got_tiles[j])
        return pltpu.make_async_remote_copy(
            src_ref=y_out.at[u, piece_at(s), at], dst_ref=y_got.at[u, piece_at(s), at],
            send_sem=y_send.at[u, s, j], recv_sem=y_recv.at[u, s, j],
            device_id=y_peer, device_id_type=MESH,
        )

    def z_copy(u, s, j, slot=None):
        at = pl.ds(*got_tiles[j])
        goal, into = beside, u
        if u < 2:
            goal = inner * target_z(u) + (1 - inner) * beside
            into = inner * last + (1 - inner) * u
        into = into if slot is None else slot
        return pltpu.make_async_remote_copy(
            src_ref=z_out.at[u, piece_at(s), at], dst_ref=z_got.at[into, piece_at(s), at],
            send_sem=z_send.at[u, s, j], recv_sem=z_recv.at[into, s, j],
            device_id=on_z(goal), device_id_type=MESH,
        )

    def peak_copy(buffer, i, partner, at):
        return pltpu.make_async_remote_copy(
            src_ref=buffer.at[0], dst_ref=buffer.at[i],
            send_sem=pk_send.at[at], recv_sem=pk_recv.at[at],
            device_id=partner, device_id_type=MESH,
        )

    core_peak = peak_copy(core_peaks, 1, sibling, 0)
    y_peak = peak_copy(y_peaks, 1, y_peer, 1)
    near_peak = peak_copy(near_peaks, 1, z_near, 2)
    far_peak = peak_copy(far_peaks, 1, z_far, 3)

    def act_peak_copy(t):
        return pltpu.make_async_remote_copy(
            src_ref=act_peaks.at[0], dst_ref=act_peaks.at[t],
            send_sem=ap_send.at[t - 1], recv_sem=ap_recv.at[t - 1],
            device_id=on_tensor(t), device_id_type=MESH,
        )

    def turn_act(u, k):
        act_load(u, k).wait()
        at = pair_cols(u, k)
        read = act_own[:, at]
        top = jnp.max(jnp.abs(read).reshape(tokens // SUBLANES, SUBLANES, CORES * block), axis=0)
        core_peaks[0, :, at] = jnp.max(top.astype(jnp.float32), axis=0, keepdims=True)
        act_down[pair_at(u, k)] = jnp.transpose(read).reshape(CORES, block, tokens)

    def send_x(u, k, s, cuts=1):
        for t in range(1, tensor):
            for cut in range(cuts):
                x_copy(t, u, k, s, cut, cuts).start()

    turn_act(*order[0][:2])
    pl.semaphore_wait(barrier, len(partners) + below + above)
    greet(far_sem)
    smalls[1].wait()
    act_tops[0] = jnp.max(act_hist[0], axis=0, keepdims=True)
    for t in range(1, tensor):
        top_copy(t).start()
    turned = {order[0][:2]}
    for u, k, s in order:
        if (u, k) not in turned:
            turn_act(u, k)
            turned.add((u, k))
        send_x(u, k, s, TAIL_CUTS if (u, k, s) == order[-1] else 1)
        if (u, k, s) == order[1]:
            for t in range(1, tensor):
                hist_copy(t, 0).start()

    smalls[0].wait()
    if rest:
        grad_scale[:, padded - LANES:] = jnp.ones((1, LANES), jnp.float32)
    grad_scale[:, :cols] = QUANT_LIMIT / jnp.maximum(
        jnp.max(grad_hist[...], axis=0, keepdims=True), SCALE_FLOOR
    )

    def quantize_cols(j):
        at = pl.ds(pl.multiple_of(j * LANES, LANES), LANES)
        scale = grad_scale[:, at]
        top = jnp.zeros((SUBLANES, LANES), jnp.bfloat16)
        for start, size in tiles(rows, TURN):
            turned = jnp.transpose(raw[at, start:start + size])
            mag = jnp.abs(turned).reshape(size // SUBLANES, SUBLANES, LANES)
            top = jnp.maximum(top, jnp.max(mag, axis=0))
            gq[start:start + size, at] = quantize(turned, scale)
        here = pl.ds(pl.multiple_of(width + j * LANES, LANES), LANES)
        core_peaks[0, :, here] = jnp.max(top.astype(jnp.float32), axis=0, keepdims=True)

    def grad_chunk(i, carry):
        grad_load(i).wait()
        quantize_cols(i)
        return carry

    lax.fori_loop(0, full, grad_chunk, 0)
    if rest:
        grad_load(full, rest).wait()
        quantize_cols(full)
    core_peak.start()
    pl.semaphore_wait(far_sem, below + above)

    smalls[2].wait()
    owner = owner_ref[...]
    top = act_tops[0]
    for t in range(1, tensor):
        top_copy(t).wait()
        top = jnp.where(owner == lax.rem(mt + tensor - t, tensor), act_tops[t], top)
    act_scale[...] = QUANT_LIMIT / jnp.maximum(top, SCALE_FLOOR)
    for start in range(0, width, LANES):
        turned = jnp.transpose(jnp.broadcast_to(act_scale[:, start:start + LANES], (LANES, LANES)))
        first = start // block
        scale_down[first:first + LANES // block] = turned.reshape(LANES // block, block, LANES)

    def load_own(u):
        at = pl.ds(target_z(u) * (ROWS_Y * CORES), ROWS_Y * CORES)
        count = ROWS_Y * CORES * block
        scale = scale_down[at].reshape(count, LANES)
        for start in range(0, tokens, LANES):
            read = act_down[at, :, start:start + LANES].reshape(count, LANES)
            own_lhs[:, start:start + LANES] = quantize(read, scale)

    def own_product(u, j):
        start, size = own_tiles[j]
        source = pl.ds(pl.multiple_of(mt * tokens, tokens), tokens)
        part[u, :, start:start + size] = jnp.dot(
            own_lhs[...], gq[source, start:start + size], preferred_element_type=jnp.float32
        )

    def got_product(u, k, s, cuts=1):
        scale = scale_down[pair_at(u, k), piece_at(s), :].reshape(CORES * piece, LANES)
        span = tokens // cuts
        for cut in range(cuts):
            first = cut * span
            for t in range(1, tensor):
                x_copy(t, u, k, s, cut, cuts).wait_recv()
                for start in range(first, first + span, LANES):
                    read = act_got[t - 1, pair_at(u, k), piece_at(s), start:start + LANES]
                    got_lhs[t - 1, :, start:start + LANES] = quantize(
                        read.reshape(CORES * piece, LANES), scale
                    )
            for j, (start, size) in enumerate(got_tiles):
                for t in range(1, tensor):
                    from_rank = lax.rem(mt + tensor - t, tensor)
                    source = pl.ds(pl.multiple_of(from_rank * tokens + first, TURN), span)
                    term = jnp.dot(
                        got_lhs[t - 1, :, first:first + span], gq[source, start:start + size],
                        preferred_element_type=jnp.float32,
                    )
                    for c in range(CORES):
                        part[u, part_rows(k, c, s), start:start + size] += term[
                            c * piece:(c + 1) * piece
                        ]
                if cut == cuts - 1:
                    core_copy(u, k, s, j).start()

    def core_sum(u, k, s, j):
        start, size = got_tiles[j]
        core_copy(u, k, s, j).wait_recv()
        return (
            part[u, part_rows(k, core, s), start:start + size]
            + core_got[step_of(u, k, s), :, start:start + size]
        )

    def send_y(u, s):
        for j, (start, size) in enumerate(got_tiles):
            y_out[u, piece_at(s), start:start + size] = core_sum(u, 0, s, j).astype(jnp.bfloat16)
            y_copy(u, s, j).start()

    def line_sum(u, s, j):
        start, size = got_tiles[j]
        return core_sum(u, 1, s, j) + y_got[u, piece_at(s), start:start + size].astype(jnp.float32)

    def send_z(u, s, add):
        for j, (start, size) in enumerate(got_tiles):
            y_copy(u, s, j).wait_recv()
            total = line_sum(u, s, j)
            if add:
                z_copy(u, s, j, u).wait_recv()
                total = total + z_got[u, piece_at(s), start:start + size].astype(jnp.float32)
            z_out[u, piece_at(s), start:start + size] = total.astype(jnp.bfloat16)
            z_copy(u, s, j).start()

    load_own(0)
    for j in range(len(own_tiles)):
        own_product(0, j)
    core_peak.wait()
    y_peaks[0] = jnp.max(core_peaks[...], axis=0)
    y_peak.start()

    def finish_line(s):
        for j, (start, size) in enumerate(got_tiles):
            y_copy(last, s, j).wait_recv()
            for u in (2, last):
                z_copy(2, s, j, u).wait_recv()
            total = line_sum(last, s, j)
            for u in (2, last):
                total = total + z_got[u, piece_at(s), start:start + size].astype(jnp.float32)
            total = total * undo[s * piece:(s + 1) * piece, :1]
            total = total * grad_undo[:, start:start + size]
            size = min(size, cols - start)
            weight_ref[piece_at(s), start:start + size] = total[:, :size]

    where = {step: i for i, step in enumerate(order)}
    fillers, sends = [[] for _ in order], [[] for _ in order]
    far_sends = [[], []]
    for u in range(last):
        first, until = where[u, 0, 0], where[u + 1, 0, 0]
        for j in range(len(own_tiles)):
            fillers[min(first + j, until - 1)].append((u + 1, j))
        for s in range(PIECES):
            if u < 2:
                far_sends[0].append((where[u, 1, s] + 2 - u, u, s))
                far_sends[1].append((where[u, 1, s] + 5 - 2 * u, u, s))
            else:
                sends[where[u, 1, s] + 1 - s].append((1, u, s))
    for u in range(depth):
        for s in range(PIECES):
            sends[where[u, 0, s] + (1 if u == 0 else 0)].append((0, u, s))
    for i, (u, k, s) in enumerate(order):
        got_product(u, k, s, TAIL_CUTS if i == len(order) - 1 else 1)
        if u < last and (u, k, s) == (u, 0, 0):
            load_own(u + 1)
        for other, j in fillers[i]:
            own_product(other, j)
        for add, plan in enumerate(far_sends):
            due = [(other, piece_of) for at, other, piece_of in plan if at == i]

            @pl.when(inner == add)
            def _(due=due, add=add):
                for other, piece_of in due:
                    send_z(other, piece_of, add)

        for kind, other, piece_of in sends[i]:
            if kind == 0:
                send_y(other, piece_of)
            else:
                send_z(other, piece_of, 0)
        if i == steps - 1:
            y_peak.wait()
            near_peaks[0] = jnp.max(y_peaks[...], axis=0)
            near_peak.start()
            pass_hist(1)
        if i == steps + 1:
            near_peak.wait()
            far_peaks[0] = jnp.max(near_peaks[...], axis=0)
            far_peak.start()
            pass_hist(2)
        if i == where[last, 0, PIECES - 1]:
            far_peak.wait()
            tops = jnp.max(far_peaks[...], axis=0)
            act_peaks[0] = tops[:, :width]
            for t in range(1, tensor):
                act_peak_copy(t).start()
            factor = 1.0 / math.sqrt(rows * dp)
            grad_undo[...] = factor / grad_scale[...]
            undo = 1.0 / scale_down[me]
            pass_hist(3)
            smalls[3].wait()
            slots = slot_ref[...]
            hist_row = lax.broadcasted_iota(jnp.int32, grad_hist.shape, 0)
            grad_slots = slots[width:width + cols]
            for t in range(1, tensor):
                first = width + t * cols
                grad_slots = jnp.where(mt == t, slots[first:first + cols], grad_slots)
            grad_hist_out[...] = jnp.where(
                hist_row == grad_slots[None, :], tops[:, width:width + cols], grad_hist[...]
            )
        if i == len(order) - 1:
            for t in range(1, tensor):
                act_peak_copy(t).wait()
            current = act_hist[0]
            for t in range(1, tensor):
                source = lax.rem(mt + tensor - t, tensor)
                current = jnp.where(owner_ref[...] == source, hist_got[t - 1], current)
            hist_row = lax.broadcasted_iota(jnp.int32, current.shape, 0)
            act_hist_out[0] = jnp.where(
                hist_row == slots[:width][None, :], jnp.max(act_peaks[...], axis=0), current
            )
            for piece_of in range(PIECES):
                finish_line(piece_of)

    for u, k, s in order:
        for t in range(1, tensor):
            cuts = TAIL_CUTS if (u, k, s) == order[-1] else 1
            for cut in range(cuts):
                x_copy(t, u, k, s, cut, cuts).wait_send()
        for j in range(len(got_tiles)):
            core_copy(u, k, s, j).wait_send()
            if k == 0:
                y_copy(u, s, j).wait_send()
            elif u < last:
                z_copy(u, s, j).wait_send()


def fused_outputs(activations, gradients, act_history, grad_history, owner_rank, history_slot):
    dp, tensor = lax.axis_size("dp"), lax.axis_size("tensor")
    tokens, width = activations.shape
    rows, cols = gradients.shape
    hist = act_history.shape[1]
    depth = dp // (CORES * ROWS_Y)
    blocks, block = dp, width // dp
    steps = depth * ROWS_Y * PIECES
    pieces = steps + TAIL_CUTS - 1
    padded = pl.cdiv(cols, LANES) * LANES
    line = ROWS_Y * CORES * block
    dma = pltpu.SemaphoreType.DMA
    vmem = pl.BlockSpec(memory_space=pltpu.VMEM)
    hbm = pl.BlockSpec(memory_space=pl.ANY)
    f32, bf16, i32 = jnp.float32, jnp.bfloat16, jnp.int32
    others = tensor - 1
    halves = len(tiles(padded, GOT_TILE))
    return pl.pallas_call(
        functools.partial(fused_kernel, dp, tensor),
        out_shape=(
            pltpu.VMEM((block, cols), f32),
            pltpu.VMEM((1, hist, width), f32),
            pltpu.VMEM((hist, cols), f32),
        ),
        in_specs=[hbm] * 6,
        out_specs=(vmem, vmem, vmem),
        scratch_shapes=[
            pltpu.VMEM((tokens, width), bf16),
            pltpu.VMEM((blocks, block, tokens), bf16),
            pltpu.VMEM((others, blocks, block, tokens), bf16),
            pltpu.VMEM((padded, rows), bf16),
            pltpu.VMEM((rows, padded), bf16),
            pltpu.VMEM((depth, line, padded), f32),
            pltpu.VMEM((steps, block // PIECES, padded), f32),
            pltpu.VMEM((depth, block, padded), bf16),
            pltpu.VMEM((depth, block, padded), bf16),
            pltpu.VMEM((depth - 1, block, padded), bf16),
            pltpu.VMEM((depth, block, padded), bf16),
            pltpu.VMEM((line, tokens), bf16),
            pltpu.VMEM((others, CORES * (block // PIECES), tokens), bf16),
            pltpu.VMEM((1, hist, width), f32),
            pltpu.VMEM((others, hist, width), f32),
            pltpu.VMEM((hist, cols), f32),
            pltpu.VMEM((1, width), i32),
            pltpu.VMEM(history_slot.shape, i32),
            pltpu.VMEM((2, 1, width + padded), f32),
            pltpu.VMEM((2, 1, width + padded), f32),
            pltpu.VMEM((2, 1, width + padded), f32),
            pltpu.VMEM((2, 1, width + padded), f32),
            pltpu.VMEM((tensor, 1, width), f32),
            pltpu.VMEM((tensor, 1, width), f32),
            pltpu.VMEM((1, width), f32),
            pltpu.VMEM((blocks, block, LANES), f32),
            pltpu.VMEM((1, padded), f32),
            pltpu.VMEM((1, padded), f32),
            pltpu.SemaphoreType.REGULAR,
            dma((depth * ROWS_Y,)), dma((padded // LANES,)), dma((4,)), dma((others, 3)), dma((others, 3)), dma((others,)), dma((others,)),
            dma((others, pieces)), dma((others, pieces)), dma((steps, halves)), dma((steps, halves)),
            dma((depth, PIECES, halves)), dma((depth, PIECES, halves)),
            dma((depth - 1, PIECES, halves)), dma((depth, PIECES, halves)),
            dma((4,)), dma((4,)), dma((others,)), dma((others,)),
        ],
        compiler_params=pltpu.CompilerParams(
            collective_id=0, has_side_effects=True, vmem_limit_bytes=61 * 1024 * 1024
        ),
    )(
        activations, gradients.T, act_history, grad_history,
        owner_rank[None, :], history_slot,
    )


def hand_over_kernel(*refs):
    sems = refs[-1]
    half = (len(refs) - 1) // 2
    copies = [
        pltpu.make_async_copy(source, target, sems.at[i])
        for i, (source, target) in enumerate(zip(refs[:half], refs[half:-1]))
    ]
    for copy in copies:
        copy.start()
    for copy in copies:
        copy.wait()


def hand_over(*results):
    vmem = pl.BlockSpec(memory_space=pltpu.VMEM)
    hbm = pl.BlockSpec(memory_space=pl.ANY)
    return pl.pallas_call(
        hand_over_kernel,
        out_shape=tuple(jax.ShapeDtypeStruct(r.shape, r.dtype) for r in results),
        in_specs=[vmem] * len(results),
        out_specs=(hbm,) * len(results),
        scratch_shapes=[pltpu.SemaphoreType.DMA((len(results),))],
        compiler_params=pltpu.CompilerParams(vmem_limit_bytes=1024 * 1024),
    )(*results)


def gathered_sums(activations, gradients, act_history, grad_history, owner_rank):
    my_rank = lax.axis_index("tensor")
    held = jnp.where(owner_rank[None, :] == my_rank, act_history[0], jnp.float32(0.0))
    current = lax.psum(held, "tensor")
    act_scale = QUANT_LIMIT / jnp.maximum(jnp.max(current, axis=0), SCALE_FLOOR)
    grad_scale = QUANT_LIMIT / jnp.maximum(jnp.max(grad_history, axis=0), SCALE_FLOOR)
    gathered_rows = lax.all_gather(quantize(activations, act_scale), "tensor", axis=0, tiled=True)
    summed = lax.psum_scatter(
        lax.dot_general(
            gathered_rows, quantize(gradients, grad_scale), (((0,), (0,)), ((), ())),
            preferred_element_type=jnp.float32,
        ),
        "dp", scatter_dimension=0, tiled=True,
    )
    act_peak = lax.pmax(jnp.max(jnp.abs(activations), axis=0).astype(jnp.float32), ("dp", "tensor"))
    grad_peak = lax.pmax(jnp.max(jnp.abs(gradients), axis=0).astype(jnp.float32), "dp")
    return summed, current, act_peak[None, :], grad_peak[None, :]


def body(activations, gradients, act_history, grad_history, owner_rank, history_slot):
    dp = lax.axis_size("dp")
    model_width = act_history.shape[2]
    column_total = gradients.shape[1]
    row_count = model_width // dp
    fits = dp == CORES * ROWS_Y * DEPTH
    fits = fits and (row_count * CORES) % LANES == 0 and row_count % (PIECES * SUBLANES) == 0
    fits = fits and model_width % (CORES * ROWS_Y * LANES) == 0 and activations.shape[0] % (TAIL_CUTS * TURN) == 0
    fits = fits and column_total % SUBLANES == 0
    if fits:
        return hand_over(*fused_outputs(
            activations, gradients, act_history, grad_history, owner_rank, history_slot
        ))
    act_slots = history_slot[:model_width]
    grad_slots = lax.dynamic_slice_in_dim(
        history_slot, model_width + lax.axis_index("tensor") * column_total, column_total, 0
    )
    summed, current, act_peak, grad_peak = gathered_sums(
        activations, gradients, act_history, grad_history, owner_rank
    )
    act_scale = QUANT_LIMIT / jnp.maximum(jnp.max(current, axis=0), SCALE_FLOOR)
    grad_scale = QUANT_LIMIT / jnp.maximum(jnp.max(grad_history, axis=0), SCALE_FLOOR)
    grad_factor = 1.0 / math.sqrt(gradients.shape[0] * dp)
    row_base = lax.axis_index("dp") * row_count
    row_scale = lax.dynamic_slice_in_dim(act_scale, row_base, row_count, 0)
    weight_grad = summed / (row_scale[:, None] * grad_scale[None, :]) * grad_factor
    act_history_out = place_peaks(current, act_peak[0], act_slots)[None]
    grad_history_out = place_peaks(grad_history, grad_peak[0], grad_slots)
    return (weight_grad, act_history_out, grad_history_out)


def solution(mesh):
    placed = (
        P(("dp", "tensor"), None),
        P("dp", "tensor"),
        P("tensor", None, None),
        P(None, "tensor"),
        P(),
        P(),
    )
    return jax.shard_map(
        body,
        mesh=mesh,
        in_specs=placed,
        out_specs=(P("dp", "tensor"), P("tensor", None, None), P(None, "tensor")),
        check_vma=False,
    )
```

```python
import functools
import math

import jax
import jax.numpy as jnp
from jax import lax
from jax.experimental import pallas as pl
from jax.experimental.pallas import tpu as pltpu
from jax.sharding import PartitionSpec as P

QUANT_LIMIT = 448.0
SCALE_FLOOR = 0.25
CORES = 2
ROWS_Y = 2
DEPTH = 4
LANES = 128
SUBLANES = 16
PIECES = 2
OWN_TILE = 768
GOT_TILE = 1536
TAIL_CUTS = 2
RING = 8
GROUP = 3
TURN = 256
MESH = pl.DeviceIdType.MESH


def quantize(values, scale):
    scaled = values.astype(jnp.float32) * scale
    return jnp.clip(scaled, -QUANT_LIMIT, QUANT_LIMIT).astype(jnp.bfloat16)


def place_peaks(history, peaks, slots):
    rows = lax.broadcasted_iota(jnp.int32, history.shape, 0)
    return jnp.where(rows == slots[None, :], peaks[None, :], history)


def tiles(width, step):
    return [(start, min(step, width - start)) for start in range(0, width, step)]


def piece_plan(block):
    size = block // PIECES
    fine = size // 2
    spans = [(i * size, size) for i in range(PIECES)]
    order = [[(u, k, s)] for u in range(DEPTH) for k in range(ROWS_Y) for s in spans]
    last = DEPTH - 1
    at = order.index([(last, 0, spans[0])])
    cuts = [(block - size + i * fine, fine) for i in range(2)]
    order[at - 1] = order[at]
    order[at:at + 2] = [[(last, 0, cut), (last - 1, 1, cut)] for cut in cuts]
    return spans, cuts, order


def fused_kernel(
    dp, tensor,
    act_hbm, grad_hbm, act_hist_hbm, grad_hist_hbm, owner_hbm, slot_hbm,
    weight_ref, act_hist_out, grad_hist_out,
    act_own, act_down, act_got, raw, gq, part, core_got, y_out, y_got, z_out, z_got,
    own_lhs, got_lhs, act_hist, hist_got, grad_hist, owner_ref, slot_ref,
    core_peaks, y_peaks, near_peaks, far_peaks, act_peaks,
    act_tops, act_scale, scale_down, grad_scale, grad_undo, far_sem,
    load_sem, grad_sem, small_sem, hist_send, hist_recv, top_send, top_recv,
    x_send, x_recv, core_send, core_recv, y_send, y_recv, z_send, z_recv,
    pk_send, pk_recv, ap_send, ap_recv,
):
    me = lax.axis_index("dp")
    mt = lax.axis_index("tensor")
    core = lax.rem(me, CORES)
    chip = lax.div(me, CORES)
    yy = lax.rem(chip, ROWS_Y)
    zz = lax.div(chip, ROWS_Y)
    depth = DEPTH
    half, odd = lax.div(zz, 2), lax.rem(zz, 2)
    inner = odd * (1 - half) + (1 - odd) * half
    beside = 2 * half + 1 - odd
    tokens, width = act_hbm.shape
    cols, rows = grad_hbm.shape
    block = width // dp
    piece = block // PIECES
    padded = grad_scale.shape[1]
    own_tiles = tiles(padded, OWN_TILE)
    got_tiles = tiles(padded, GOT_TILE)
    steps = ROWS_Y * PIECES
    last = depth - 1
    spans, cut_spans, order = piece_plan(block)
    number = {step: i for i, step in enumerate(step for group in order for step in group)}
    last_spans = spans[:-1] + cut_spans

    def dp_index(z, y, c):
        return (z * ROWS_Y + y) * CORES + c

    def on_tensor(t):
        return {"tensor": lax.rem(mt + t, tensor)}

    sibling = {"dp": dp_index(zz, yy, 1 - core)}
    y_peer = {"dp": dp_index(zz, 1 - yy, core)}

    def on_z(z):
        return {"dp": dp_index(z, yy, core)}

    z_near, z_far = on_z(beside), on_z(2 * (1 - half) + odd)

    barrier = pltpu.get_barrier_semaphore()
    partners = [on_tensor(t) for t in range(1, tensor)] + [sibling, y_peer]
    below = lax.div(zz + depth - 1, depth)
    above = 1 - lax.div(zz + 1, depth)

    def greet(semaphore):
        @pl.when(zz > 0)
        def _():
            pl.semaphore_signal(semaphore, inc=1, device_id=on_z(zz - 1), device_id_type=MESH)

        @pl.when(zz < depth - 1)
        def _():
            pl.semaphore_signal(semaphore, inc=1, device_id=on_z(zz + 1), device_id_type=MESH)

    for partner in partners:
        pl.semaphore_signal(barrier, inc=1, device_id=partner, device_id_type=MESH)
    greet(barrier)

    def target_z(u):
        return (3 * (1 - half), 2 - half, beside, zz)[u]

    def side(k):
        return yy * k + (1 - yy) * (1 - k)

    def pair_of(u, k):
        return target_z(u) * ROWS_Y + side(k)

    def pair_at(u, k):
        return pl.ds(pair_of(u, k) * CORES, CORES)

    def pair_cols(u, k):
        return pl.ds(pl.multiple_of(pair_of(u, k) * (CORES * block), LANES), CORES * block)

    def act_load(u, k):
        at = pair_cols(u, k)
        return pltpu.make_async_copy(
            act_hbm.at[:, at], act_own.at[:, at], load_sem.at[min(u * ROWS_Y + k, 1)]
        )

    def act_rest():
        at = pl.ds(0, width - CORES * block)
        return pltpu.make_async_copy(act_hbm.at[:, at], act_own.at[:, at], load_sem.at[1])

    for u in range(depth):
        for k in range(ROWS_Y):
            act_load(u, k).start()
    smalls = [
        pltpu.make_async_copy(source, target, small_sem.at[i])
        for i, (source, target) in enumerate((
            (grad_hist_hbm, grad_hist), (act_hist_hbm, act_hist),
            (owner_hbm, owner_ref), (slot_hbm, slot_ref),
        ))
    ]
    for small in smalls:
        small.start()

    group = GROUP * LANES
    groups, rest = cols // group, cols % group

    def grad_load(i, size=group):
        at = pl.ds(i * group, size)
        return pltpu.make_async_copy(grad_hbm.at[at], raw.at[at], grad_sem.at[i])

    def start_load(i, carry):
        grad_load(i).start()
        return carry

    lax.fori_loop(0, groups, start_load, 0)
    if rest:
        grad_load(groups, rest).start()
    if padded > cols:
        raw[cols:, :] = jnp.zeros((padded - cols, rows), jnp.bfloat16)

    def piece_at(s):
        return pl.ds(*s)

    def part_rows(k, c, s):
        return pl.ds(pl.multiple_of((side(k) * CORES + c) * block + s[0], s[1]), s[1])

    def hist_copy(t, stage):
        parts = CORES if stage == 2 else CORES * ROWS_Y
        mine = core if stage == 2 else core * ROWS_Y + yy
        at = pl.ds(pl.multiple_of(mine * (width // parts), LANES), width // parts)
        held = hist_got.at[t - 1, :, at]
        return pltpu.make_async_remote_copy(
            src_ref=held if stage else act_hist_hbm.at[0, :, at], dst_ref=held,
            send_sem=hist_send.at[t - 1], recv_sem=hist_recv.at[t - 1, stage],
            device_id=(on_tensor(t), y_peer, sibling)[stage], device_id_type=MESH,
        )

    def top_copy(t):
        return pltpu.make_async_remote_copy(
            src_ref=act_tops.at[0], dst_ref=act_tops.at[t],
            send_sem=top_send.at[t - 1], recv_sem=top_recv.at[t - 1],
            device_id=on_tensor(t), device_id_type=MESH,
        )

    def pass_hist(stage):
        for t in range(1, tensor):
            hist_copy(t, stage - 1).wait()
            if stage < 3:
                hist_copy(t, stage).start()

    def x_copy(t, u, k, s, cut=0, cuts=1):
        at = number[u, k, s] + cut
        span = pl.ds(cut * (tokens // cuts), tokens // cuts)
        return pltpu.make_async_remote_copy(
            src_ref=act_down.at[pair_at(u, k), piece_at(s), span],
            dst_ref=act_got.at[t - 1, pair_at(u, k), piece_at(s), span],
            send_sem=x_send.at[t - 1], recv_sem=x_recv.at[t - 1, at],
            device_id=on_tensor(t), device_id_type=MESH,
        )

    def core_copy(u, k, s, j):
        at = number[u, k, s]
        start, size = got_tiles[j]
        return pltpu.make_async_remote_copy(
            src_ref=part.at[u, part_rows(k, 1 - core, s), pl.ds(start, size)],
            dst_ref=core_got.at[at, pl.ds(0, s[1]), pl.ds(start, size)],
            send_sem=core_send, recv_sem=core_recv.at[at % RING, j],
            device_id=sibling, device_id_type=MESH,
        )

    whole = [(0, padded)]

    def y_copy(u, s, j=0):
        at = pl.ds(*(got_tiles if u == last else whole)[j])
        index = u * PIECES + spans.index(s) if u < last else (
            last * PIECES + last_spans.index(s) * len(got_tiles) + j
        )
        return pltpu.make_async_remote_copy(
            src_ref=y_out.at[u, piece_at(s), at], dst_ref=y_got.at[u, piece_at(s), at],
            send_sem=y_send, recv_sem=y_recv.at[index],
            device_id=y_peer, device_id_type=MESH,
        )

    def z_copy(u, s, j=0, slot=None):
        at = pl.ds(*(got_tiles if u == 2 else whole)[j])
        goal, into, index = beside, u, last * PIECES + j
        if u < 2:
            goal = inner * target_z(u) + (1 - inner) * beside
            into = inner * last + (1 - inner) * u
            into = into if slot is None else slot
            index = (inner * 2 + (1 - inner) * u if slot is None else min(slot, 2)) * PIECES
            index = index + spans.index(s)
        else:
            index += last_spans.index(s) * len(got_tiles)
        return pltpu.make_async_remote_copy(
            src_ref=z_out.at[u, piece_at(s), at], dst_ref=z_got.at[into, piece_at(s), at],
            send_sem=z_send, recv_sem=z_recv.at[index],
            device_id=on_z(goal), device_id_type=MESH,
        )

    def peak_copy(buffer, i, partner, at):
        return pltpu.make_async_remote_copy(
            src_ref=buffer.at[0], dst_ref=buffer.at[i],
            send_sem=pk_send, recv_sem=pk_recv.at[at],
            device_id=partner, device_id_type=MESH,
        )

    core_peak = peak_copy(core_peaks, 1, sibling, 0)
    y_peak = peak_copy(y_peaks, 1, y_peer, 1)
    near_peak = peak_copy(near_peaks, 1, z_near, 2)
    far_peak = peak_copy(far_peaks, 1, z_far, 3)

    def act_peak_copy(t):
        return pltpu.make_async_remote_copy(
            src_ref=act_peaks.at[0], dst_ref=act_peaks.at[t],
            send_sem=ap_send.at[t - 1], recv_sem=ap_recv.at[t - 1],
            device_id=on_tensor(t), device_id_type=MESH,
        )

    def turn_act(u, k):
        at = pair_cols(u, k)
        read = act_own[:, at]
        top = jnp.max(jnp.abs(read).reshape(tokens // SUBLANES, SUBLANES, CORES * block), axis=0)
        core_peaks[0, :, at] = jnp.max(top.astype(jnp.float32), axis=0, keepdims=True)
        act_down[pair_at(u, k)] = jnp.transpose(read).reshape(CORES, block, tokens)

    def send_x(u, k, s, cuts=1):
        for t in range(1, tensor):
            for cut in range(cuts):
                x_copy(t, u, k, s, cut, cuts).start()

    act_load(0, 0).wait()
    turn_act(0, 0)
    pl.semaphore_wait(barrier, len(partners) + below + above)
    greet(far_sem)
    smalls[1].wait()
    act_tops[0] = jnp.max(act_hist[0], axis=0, keepdims=True)
    for t in range(1, tensor):
        top_copy(t).start()
    turned = {(0, 0)}
    for u, k, s in number:
        if (u, k) not in turned:
            if len(turned) == 1:
                act_rest().wait()
            turn_act(u, k)
            turned.add((u, k))
        send_x(u, k, s, TAIL_CUTS if number[u, k, s] == len(number) - 1 else 1)
        if number[u, k, s] == 1:
            for t in range(1, tensor):
                hist_copy(t, 0).start()

    smalls[0].wait()
    if padded > cols:
        grad_scale[:, padded - LANES:] = jnp.ones((1, LANES), jnp.float32)
    grad_scale[:, :cols] = QUANT_LIMIT / jnp.maximum(
        jnp.max(grad_hist[...], axis=0, keepdims=True), SCALE_FLOOR
    )

    def quantize_cols(j):
        at = pl.ds(pl.multiple_of(j * LANES, LANES), LANES)
        scale = grad_scale[:, at]
        top = jnp.zeros((SUBLANES, LANES), jnp.bfloat16)
        for start, size in tiles(rows, TURN):
            turned = jnp.transpose(raw[at, start:start + size])
            mag = jnp.abs(turned).reshape(size // SUBLANES, SUBLANES, LANES)
            top = jnp.maximum(top, jnp.max(mag, axis=0))
            gq[start:start + size, at] = quantize(turned, scale)
        here = pl.ds(pl.multiple_of(width + j * LANES, LANES), LANES)
        core_peaks[0, :, here] = jnp.max(top.astype(jnp.float32), axis=0, keepdims=True)

    def grad_chunk(i, carry):
        grad_load(i).wait()
        for j in range(GROUP):
            quantize_cols(i * GROUP + j)
        return carry

    lax.fori_loop(0, groups, grad_chunk, 0)
    if rest:
        grad_load(groups, rest).wait()
        for j in range(pl.cdiv(rest, LANES)):
            quantize_cols(groups * GROUP + j)
    core_peak.start()
    pl.semaphore_wait(far_sem, below + above)

    smalls[2].wait()
    owner = owner_ref[...]
    top = act_tops[0]
    for t in range(1, tensor):
        top_copy(t).wait()
        top = jnp.where(owner == lax.rem(mt + tensor - t, tensor), act_tops[t], top)
    act_scale[...] = QUANT_LIMIT / jnp.maximum(top, SCALE_FLOOR)
    for start in range(0, width, LANES):
        turned = jnp.transpose(jnp.broadcast_to(act_scale[:, start:start + LANES], (LANES, LANES)))
        first = start // block
        scale_down[first:first + LANES // block] = turned.reshape(LANES // block, block, LANES)

    def load_own(u):
        at = pl.ds(target_z(u) * (ROWS_Y * CORES), ROWS_Y * CORES)
        count = ROWS_Y * CORES * block
        scale = scale_down[at].reshape(count, LANES)
        for start in range(0, tokens, LANES):
            read = act_down[at, :, start:start + LANES].reshape(count, LANES)
            own_lhs[:, start:start + LANES] = quantize(read, scale)

    def own_product(u, j):
        start, size = own_tiles[j]
        source = pl.ds(pl.multiple_of(mt * tokens, tokens), tokens)
        part[u, :, start:start + size] = jnp.dot(
            own_lhs[...], gq[source, start:start + size], preferred_element_type=jnp.float32
        )

    def got_product(group, cuts=1):
        span = tokens // cuts
        places, total = [], 0
        for u, k, s in group:
            places.append((u, k, s, total))
            total += CORES * s[1]
        for cut in range(cuts):
            first = cut * span
            for u, k, s, base in places:
                count = CORES * s[1]
                scale = scale_down[pair_at(u, k), piece_at(s), :].reshape(count, LANES)
                for t in range(1, tensor):
                    x_copy(t, u, k, s, cut, cuts).wait_recv()
                    for start in range(first, first + span, LANES):
                        read = act_got[t - 1, pair_at(u, k), piece_at(s), start:start + LANES]
                        got_lhs[t - 1, base:base + count, start:start + LANES] = quantize(
                            read.reshape(count, LANES), scale
                        )
            for j, (start, size) in enumerate(got_tiles):
                for t in range(1, tensor):
                    from_rank = lax.rem(mt + tensor - t, tensor)
                    source = pl.ds(pl.multiple_of(from_rank * tokens + first, TURN), span)
                    term = jnp.dot(
                        got_lhs[t - 1, :total, first:first + span],
                        gq[source, start:start + size], preferred_element_type=jnp.float32,
                    )
                    for u, k, s, base in places:
                        for c in range(CORES):
                            at = base + c * s[1]
                            part[u, part_rows(k, c, s), start:start + size] += term[at:at + s[1]]
                if cut == cuts - 1:
                    for u, k, s in group:
                        core_copy(u, k, s, j).start()

    def core_sum(u, k, s, j):
        start, size = got_tiles[j]
        core_copy(u, k, s, j).wait_recv()
        return (
            part[u, part_rows(k, core, s), start:start + size]
            + core_got[number[u, k, s], :s[1], start:start + size]
        )

    def send_y(u, s):
        for j, (start, size) in enumerate(got_tiles):
            y_out[u, piece_at(s), start:start + size] = core_sum(u, 0, s, j).astype(jnp.bfloat16)
            if u == last or j == len(got_tiles) - 1:
                y_copy(u, s, j if u == last else 0).start()

    def line_sum(u, s, j):
        start, size = got_tiles[j]
        return core_sum(u, 1, s, j) + y_got[u, piece_at(s), start:start + size].astype(jnp.float32)

    def send_z(u, s, add):
        if u < last - 1 or s != cut_spans[1]:
            y_copy(u, spans[s[0] // piece]).wait_recv()
        if add:
            z_copy(u, s, 0, u).wait_recv()
        for j, (start, size) in enumerate(got_tiles):
            total = line_sum(u, s, j)
            if add:
                total = total + z_got[u, piece_at(s), start:start + size].astype(jnp.float32)
            z_out[u, piece_at(s), start:start + size] = total.astype(jnp.bfloat16)
            if u == 2 or j == len(got_tiles) - 1:
                z_copy(u, s, j if u == 2 else 0).start()

    load_own(0)
    for j in range(len(own_tiles)):
        own_product(0, j)
    core_peak.wait()
    y_peaks[0] = jnp.max(core_peaks[...], axis=0)
    y_peak.start()

    def finish_line(s):
        z_copy(0, s, 0, last).wait_recv()
        for j, (start, size) in enumerate(got_tiles):
            for part_of in last_spans:
                if s[0] <= part_of[0] < s[0] + s[1]:
                    z_copy(last - 1, part_of, j).wait_recv()
                    y_copy(last, part_of, j).wait_recv()
            total = line_sum(last, s, j)
            for u in (2, last):
                total = total + z_got[u, piece_at(s), start:start + size].astype(jnp.float32)
            total = total * undo[s[0]:s[0] + s[1], :1]
            total = total * grad_undo[:, start:start + size]
            size = min(size, cols - start)
            weight_ref[piece_at(s), start:start + size] = total[:, :size]

    where = {step: i for i, group in enumerate(order) for step in group}
    fillers, sends = [[] for _ in order], [[] for _ in order]
    far_sends = [[], []]
    for u, k, s in number:
        i = where[u, k, s]
        if k == 0:
            sends[i + (1 if u == 0 else 0)].append((0, u, s))
        elif u < 2:
            far_sends[0].append((i + 2 - u, u, s))
            far_sends[1].append((i + 5 - 2 * u, u, s))
        elif u == 2:
            sends[i if s in cut_spans else i + 1].append((1, u, s))
    starts = [where[u, 0, spans[0]] for u in range(depth)]
    for u in range(last):
        for j in range(len(own_tiles)):
            fillers[min(starts[u] + j, starts[u + 1] - 1)].append((u + 1, j))
    for i, group in enumerate(order):
        got_product(group, TAIL_CUTS if i == len(order) - 1 else 1)
        if i in starts[:last]:
            load_own(starts.index(i) + 1)
        for other, j in fillers[i]:
            own_product(other, j)
        for add, plan in enumerate(far_sends):
            due = [(other, piece_of) for at, other, piece_of in plan if at == i]

            @pl.when(inner == add)
            def _(due=due, add=add):
                for other, piece_of in due:
                    send_z(other, piece_of, add)

        for kind, other, piece_of in sends[i]:
            if kind == 0:
                send_y(other, piece_of)
            else:
                send_z(other, piece_of, 0)
        if i == steps - 1:
            y_peak.wait()
            near_peaks[0] = jnp.max(y_peaks[...], axis=0)
            near_peak.start()
            pass_hist(1)
        if i == steps + 1:
            near_peak.wait()
            far_peaks[0] = jnp.max(near_peaks[...], axis=0)
            far_peak.start()
            pass_hist(2)
        if i == where[last, 0, cut_spans[1]]:
            far_peak.wait()
            tops = jnp.max(far_peaks[...], axis=0)
            act_peaks[0] = tops[:, :width]
            for t in range(1, tensor):
                act_peak_copy(t).start()
            factor = 1.0 / math.sqrt(rows * dp)
            grad_undo[...] = factor / grad_scale[...]
            undo = 1.0 / scale_down[me]
            pass_hist(3)
            smalls[3].wait()
            slots = slot_ref[...]
            hist_row = lax.broadcasted_iota(jnp.int32, grad_hist.shape, 0)
            grad_slots = slots[width:width + cols]
            for t in range(1, tensor):
                first = width + t * cols
                grad_slots = jnp.where(mt == t, slots[first:first + cols], grad_slots)
            grad_hist_out[...] = jnp.where(
                hist_row == grad_slots[None, :], tops[:, width:width + cols], grad_hist[...]
            )
        if i == len(order) - 1:
            for t in range(1, tensor):
                act_peak_copy(t).wait()
            current = act_hist[0]
            for t in range(1, tensor):
                source = lax.rem(mt + tensor - t, tensor)
                current = jnp.where(owner_ref[...] == source, hist_got[t - 1], current)
            hist_row = lax.broadcasted_iota(jnp.int32, current.shape, 0)
            act_hist_out[0] = jnp.where(
                hist_row == slots[:width][None, :], jnp.max(act_peaks[...], axis=0), current
            )
            for span in spans:
                finish_line(span)

    def all_sent(held, semaphore):
        pltpu.make_async_remote_copy(
            src_ref=held, dst_ref=held, send_sem=semaphore, recv_sem=semaphore,
            device_id=sibling, device_id_type=MESH,
        ).wait_send()

    for t in range(1, tensor):
        all_sent(act_down, x_send.at[t - 1])
    all_sent(part.at[pl.ds(0, depth // CORES)], core_send)
    all_sent(y_out, y_send)
    all_sent(z_out, z_send)


def fused_outputs(activations, gradients, act_history, grad_history, owner_rank, history_slot):
    dp, tensor = lax.axis_size("dp"), lax.axis_size("tensor")
    tokens, width = activations.shape
    rows, cols = gradients.shape
    hist = act_history.shape[1]
    depth = dp // (CORES * ROWS_Y)
    blocks, block = dp, width // dp
    steps = sum(len(group) for group in piece_plan(block)[2])
    pieces = steps + TAIL_CUTS - 1
    hops = (depth - 1) * PIECES + (PIECES + 1) * len(tiles(pl.cdiv(cols, LANES) * LANES, GOT_TILE))
    padded = pl.cdiv(cols, LANES) * LANES
    line = ROWS_Y * CORES * block
    dma = pltpu.SemaphoreType.DMA
    vmem = pl.BlockSpec(memory_space=pltpu.VMEM)
    hbm = pl.BlockSpec(memory_space=pl.ANY)
    f32, bf16, i32 = jnp.float32, jnp.bfloat16, jnp.int32
    others = tensor - 1
    halves = len(tiles(padded, GOT_TILE))
    loads = pl.cdiv(cols, GROUP * LANES)
    return pl.pallas_call(
        functools.partial(fused_kernel, dp, tensor),
        out_shape=(
            pltpu.VMEM((block, cols), f32),
            pltpu.VMEM((1, hist, width), f32),
            pltpu.VMEM((hist, cols), f32),
        ),
        in_specs=[hbm] * 6,
        out_specs=(vmem, vmem, vmem),
        scratch_shapes=[
            pltpu.VMEM((tokens, width), bf16),
            pltpu.VMEM((blocks, block, tokens), bf16),
            pltpu.VMEM((others, blocks, block, tokens), bf16),
            pltpu.VMEM((padded, rows), bf16),
            pltpu.VMEM((rows, padded), bf16),
            pltpu.VMEM((depth, line, padded), f32),
            pltpu.VMEM((steps, block // PIECES, padded), f32),
            pltpu.VMEM((depth, block, padded), bf16),
            pltpu.VMEM((depth, block, padded), bf16),
            pltpu.VMEM((depth - 1, block, padded), bf16),
            pltpu.VMEM((depth, block, padded), bf16),
            pltpu.VMEM((line, tokens), bf16),
            pltpu.VMEM((others, CORES * (block // PIECES), tokens), bf16),
            pltpu.VMEM((1, hist, width), f32),
            pltpu.VMEM((others, hist, width), f32),
            pltpu.VMEM((hist, cols), f32),
            pltpu.VMEM((1, width), i32),
            pltpu.VMEM(history_slot.shape, i32),
            pltpu.VMEM((2, 1, width + padded), f32),
            pltpu.VMEM((2, 1, width + padded), f32),
            pltpu.VMEM((2, 1, width + padded), f32),
            pltpu.VMEM((2, 1, width + padded), f32),
            pltpu.VMEM((tensor, 1, width), f32),
            pltpu.VMEM((tensor, 1, width), f32),
            pltpu.VMEM((1, width), f32),
            pltpu.VMEM((blocks, block, LANES), f32),
            pltpu.VMEM((1, padded), f32),
            pltpu.VMEM((1, padded), f32),
            pltpu.SemaphoreType.REGULAR,
            dma((2,)), dma((loads,)), dma((4,)),
            dma((others,)), dma((others, 3)), dma((others,)), dma((others,)),
            dma((others,)), dma((others, pieces)), dma, dma((RING, halves)),
            dma, dma((hops,)), dma, dma((hops,)),
            dma, dma((4,)), dma((others,)), dma((others,)),
        ],
        compiler_params=pltpu.CompilerParams(
            collective_id=0, has_side_effects=True, vmem_limit_bytes=61 * 1024 * 1024
        ),
    )(
        activations, gradients.T, act_history, grad_history,
        owner_rank[None, :], history_slot,
    )


def hand_over_kernel(*refs):
    sems = refs[-1]
    half = (len(refs) - 1) // 2
    copies = [
        pltpu.make_async_copy(source, target, sems.at[i])
        for i, (source, target) in enumerate(zip(refs[:half], refs[half:-1]))
    ]
    for copy in copies:
        copy.start()
    for copy in copies:
        copy.wait()


def hand_over(*results):
    vmem = pl.BlockSpec(memory_space=pltpu.VMEM)
    hbm = pl.BlockSpec(memory_space=pl.ANY)
    return pl.pallas_call(
        hand_over_kernel,
        out_shape=tuple(jax.ShapeDtypeStruct(r.shape, r.dtype) for r in results),
        in_specs=[vmem] * len(results),
        out_specs=(hbm,) * len(results),
        scratch_shapes=[pltpu.SemaphoreType.DMA((len(results),))],
        compiler_params=pltpu.CompilerParams(vmem_limit_bytes=1024 * 1024),
    )(*results)


def gathered_sums(activations, gradients, act_history, grad_history, owner_rank):
    my_rank = lax.axis_index("tensor")
    held = jnp.where(owner_rank[None, :] == my_rank, act_history[0], jnp.float32(0.0))
    current = lax.psum(held, "tensor")
    act_scale = QUANT_LIMIT / jnp.maximum(jnp.max(current, axis=0), SCALE_FLOOR)
    grad_scale = QUANT_LIMIT / jnp.maximum(jnp.max(grad_history, axis=0), SCALE_FLOOR)
    gathered_rows = lax.all_gather(quantize(activations, act_scale), "tensor", axis=0, tiled=True)
    summed = lax.psum_scatter(
        lax.dot_general(
            gathered_rows, quantize(gradients, grad_scale), (((0,), (0,)), ((), ())),
            preferred_element_type=jnp.float32,
        ),
        "dp", scatter_dimension=0, tiled=True,
    )
    act_peak = lax.pmax(jnp.max(jnp.abs(activations), axis=0).astype(jnp.float32), ("dp", "tensor"))
    grad_peak = lax.pmax(jnp.max(jnp.abs(gradients), axis=0).astype(jnp.float32), "dp")
    return summed, current, act_peak[None, :], grad_peak[None, :]


def body(activations, gradients, act_history, grad_history, owner_rank, history_slot):
    dp = lax.axis_size("dp")
    model_width = act_history.shape[2]
    column_total = gradients.shape[1]
    row_count = model_width // dp
    fits = dp == CORES * ROWS_Y * DEPTH
    fits = fits and (row_count * CORES) % LANES == 0 and row_count % (PIECES * 2 * SUBLANES) == 0
    fits = fits and model_width % (CORES * ROWS_Y * LANES) == 0 and activations.shape[0] % (TAIL_CUTS * TURN) == 0
    fits = fits and column_total % SUBLANES == 0
    if fits:
        return hand_over(*fused_outputs(
            activations, gradients, act_history, grad_history, owner_rank, history_slot
        ))
    act_slots = history_slot[:model_width]
    grad_slots = lax.dynamic_slice_in_dim(
        history_slot, model_width + lax.axis_index("tensor") * column_total, column_total, 0
    )
    summed, current, act_peak, grad_peak = gathered_sums(
        activations, gradients, act_history, grad_history, owner_rank
    )
    act_scale = QUANT_LIMIT / jnp.maximum(jnp.max(current, axis=0), SCALE_FLOOR)
    grad_scale = QUANT_LIMIT / jnp.maximum(jnp.max(grad_history, axis=0), SCALE_FLOOR)
    grad_factor = 1.0 / math.sqrt(gradients.shape[0] * dp)
    row_base = lax.axis_index("dp") * row_count
    row_scale = lax.dynamic_slice_in_dim(act_scale, row_base, row_count, 0)
    weight_grad = summed / (row_scale[:, None] * grad_scale[None, :]) * grad_factor
    act_history_out = place_peaks(current, act_peak[0], act_slots)[None]
    grad_history_out = place_peaks(grad_history, grad_peak[0], grad_slots)
    return (weight_grad, act_history_out, grad_history_out)


def solution(mesh):
    placed = (
        P(("dp", "tensor"), None),
        P("dp", "tensor"),
        P("tensor", None, None),
        P(None, "tensor"),
        P(),
        P(),
    )
    return jax.shard_map(
        body,
        mesh=mesh,
        in_specs=placed,
        out_specs=(P("dp", "tensor"), P("tensor", None, None), P(None, "tensor")),
        check_vma=False,
    )
```

```python
import functools
import math

import jax
import jax.numpy as jnp
from jax import lax
from jax.experimental import pallas as pl
from jax.experimental.pallas import tpu as pltpu
from jax.sharding import PartitionSpec as P

QUANT_LIMIT = 448.0
SCALE_FLOOR = 0.25
CORES = 2
ROWS_Y = 2
DEPTH = 4
LANES = 128
SUBLANES = 16
PIECES = 2
OWN_TILE = 768
GOT_TILE = 1536
TAIL_CUTS = 2
TAIL_STEPS = 2
RING = 8
GROUP = 3
TURN = 256
MESH = pl.DeviceIdType.MESH


def quantize(values, scale):
    scaled = values.astype(jnp.float32) * scale
    return jnp.clip(scaled, -QUANT_LIMIT, QUANT_LIMIT).astype(jnp.bfloat16)


def place_peaks(history, peaks, slots):
    rows = lax.broadcasted_iota(jnp.int32, history.shape, 0)
    return jnp.where(rows == slots[None, :], peaks[None, :], history)


def tiles(width, step):
    return [(start, min(step, width - start)) for start in range(0, width, step)]


def piece_plan(block):
    size = block // PIECES
    fine = size // 2
    spans = [(i * size, size) for i in range(PIECES)]
    order = [[(u, k, s)] for u in range(DEPTH) for k in range(ROWS_Y) for s in spans]
    last = DEPTH - 1
    at = order.index([(last, 0, spans[0])])
    cuts = [(block - size + i * fine, fine) for i in range(2)]
    order[at - 1] = order[at]
    order[at:at + 2] = [[(last, 0, cut), (last - 1, 1, cut)] for cut in cuts]
    return spans, cuts, order


def x_plan(order):
    slots, cuts_at, free = {}, [], 0
    for i, group in enumerate(order):
        cuts_at.append(TAIL_CUTS if i >= len(order) - TAIL_STEPS else 1)
        for step in group:
            slots[step] = free
            free += cuts_at[-1]
    return slots, cuts_at


def fused_kernel(
    dp, tensor,
    act_hbm, grad_hbm, act_hist_hbm, grad_hist_hbm, owner_hbm, slot_hbm,
    weight_ref, act_hist_out, grad_hist_out,
    act_own, act_down, act_got, raw, gq, part, core_got, y_out, y_got, z_out, z_got,
    own_lhs, got_lhs, act_hist, hist_got, grad_hist, owner_ref, slot_ref,
    core_peaks, y_peaks, near_peaks, far_peaks, act_peaks,
    act_tops, act_scale, scale_down, grad_scale, grad_undo, far_sem,
    load_sem, grad_sem, small_sem, hist_send, hist_recv, top_send, top_recv,
    x_send, x_recv, core_send, core_recv, y_send, y_recv, z_send, z_recv,
    pk_send, pk_recv, ap_send, ap_recv,
):
    me = lax.axis_index("dp")
    mt = lax.axis_index("tensor")
    core = lax.rem(me, CORES)
    chip = lax.div(me, CORES)
    yy = lax.rem(chip, ROWS_Y)
    zz = lax.div(chip, ROWS_Y)
    depth = DEPTH
    half, odd = lax.div(zz, 2), lax.rem(zz, 2)
    inner = odd * (1 - half) + (1 - odd) * half
    beside = 2 * half + 1 - odd
    tokens, width = act_hbm.shape
    cols, rows = grad_hbm.shape
    block = width // dp
    piece = block // PIECES
    padded = grad_scale.shape[1]
    own_tiles = tiles(padded, OWN_TILE)
    got_tiles = tiles(padded, GOT_TILE)
    steps = ROWS_Y * PIECES
    last = depth - 1
    spans, cut_spans, order = piece_plan(block)
    number = {step: i for i, step in enumerate(step for group in order for step in group)}
    last_spans = spans[:-1] + cut_spans
    x_slots, cuts_at = x_plan(order)

    def dp_index(z, y, c):
        return (z * ROWS_Y + y) * CORES + c

    def on_tensor(t):
        return {"tensor": lax.rem(mt + t, tensor)}

    sibling = {"dp": dp_index(zz, yy, 1 - core)}
    y_peer = {"dp": dp_index(zz, 1 - yy, core)}

    def on_z(z):
        return {"dp": dp_index(z, yy, core)}

    z_near, z_far = on_z(beside), on_z(2 * (1 - half) + odd)

    barrier = pltpu.get_barrier_semaphore()
    partners = [on_tensor(t) for t in range(1, tensor)] + [sibling, y_peer]
    below = lax.div(zz + depth - 1, depth)
    above = 1 - lax.div(zz + 1, depth)

    def greet(semaphore):
        @pl.when(zz > 0)
        def _():
            pl.semaphore_signal(semaphore, inc=1, device_id=on_z(zz - 1), device_id_type=MESH)

        @pl.when(zz < depth - 1)
        def _():
            pl.semaphore_signal(semaphore, inc=1, device_id=on_z(zz + 1), device_id_type=MESH)

    for partner in partners:
        pl.semaphore_signal(barrier, inc=1, device_id=partner, device_id_type=MESH)
    greet(barrier)

    def target_z(u):
        return (3 * (1 - half), 2 - half, beside, zz)[u]

    def side(k):
        return yy * k + (1 - yy) * (1 - k)

    def pair_of(u, k):
        return target_z(u) * ROWS_Y + side(k)

    def pair_at(u, k):
        return pl.ds(pair_of(u, k) * CORES, CORES)

    def pair_cols(u, k):
        return pl.ds(pl.multiple_of(pair_of(u, k) * (CORES * block), LANES), CORES * block)

    def act_load(u, k):
        at = pair_cols(u, k)
        return pltpu.make_async_copy(
            act_hbm.at[:, at], act_own.at[:, at], load_sem.at[min(u * ROWS_Y + k, 1)]
        )

    def act_rest():
        at = pl.ds(0, width - CORES * block)
        return pltpu.make_async_copy(act_hbm.at[:, at], act_own.at[:, at], load_sem.at[1])

    for u in range(depth):
        for k in range(ROWS_Y):
            act_load(u, k).start()
    smalls = [
        pltpu.make_async_copy(source, target, small_sem.at[i])
        for i, (source, target) in enumerate((
            (grad_hist_hbm, grad_hist), (act_hist_hbm, act_hist),
            (owner_hbm, owner_ref), (slot_hbm, slot_ref),
        ))
    ]
    for small in smalls:
        small.start()

    wide = GROUP * LANES
    groups, rest = cols // wide, cols % wide

    def grad_load(i, size=wide):
        at = pl.ds(i * wide, size)
        return pltpu.make_async_copy(grad_hbm.at[at], raw.at[at], grad_sem.at[i])

    def start_load(i, carry):
        grad_load(i).start()
        return carry

    lax.fori_loop(0, groups, start_load, 0)
    if rest:
        grad_load(groups, rest).start()
    if padded > cols:
        raw[cols:, :] = jnp.zeros((padded - cols, rows), jnp.bfloat16)

    def piece_at(s):
        return pl.ds(*s)

    def part_rows(k, c, s):
        return pl.ds(pl.multiple_of((side(k) * CORES + c) * block + s[0], s[1]), s[1])

    def hist_copy(t, stage):
        parts = CORES if stage == 2 else CORES * ROWS_Y
        mine = core if stage == 2 else core * ROWS_Y + yy
        at = pl.ds(pl.multiple_of(mine * (width // parts), LANES), width // parts)
        held = hist_got.at[t - 1, :, at]
        return pltpu.make_async_remote_copy(
            src_ref=held if stage else act_hist_hbm.at[0, :, at], dst_ref=held,
            send_sem=hist_send.at[t - 1], recv_sem=hist_recv.at[t - 1, stage],
            device_id=(on_tensor(t), y_peer, sibling)[stage], device_id_type=MESH,
        )

    def top_copy(t):
        return pltpu.make_async_remote_copy(
            src_ref=act_tops.at[0], dst_ref=act_tops.at[t],
            send_sem=top_send.at[t - 1], recv_sem=top_recv.at[t - 1],
            device_id=on_tensor(t), device_id_type=MESH,
        )

    def pass_hist(stage):
        for t in range(1, tensor):
            hist_copy(t, stage - 1).wait()
            if stage < 3:
                hist_copy(t, stage).start()

    def x_copy(t, u, k, s, cut=0, cuts=1):
        at = x_slots[u, k, s] + cut
        span = pl.ds(cut * (tokens // cuts), tokens // cuts)
        return pltpu.make_async_remote_copy(
            src_ref=act_down.at[pair_at(u, k), piece_at(s), span],
            dst_ref=act_got.at[t - 1, pair_at(u, k), piece_at(s), span],
            send_sem=x_send.at[t - 1], recv_sem=x_recv.at[t - 1, at],
            device_id=on_tensor(t), device_id_type=MESH,
        )

    def core_copy(u, k, s, j):
        at = number[u, k, s]
        start, size = got_tiles[j]
        return pltpu.make_async_remote_copy(
            src_ref=part.at[u, part_rows(k, 1 - core, s), pl.ds(start, size)],
            dst_ref=core_got.at[at, pl.ds(0, s[1]), pl.ds(start, size)],
            send_sem=core_send, recv_sem=core_recv.at[at % RING, j],
            device_id=sibling, device_id_type=MESH,
        )

    whole = [(0, padded)]

    def y_copy(u, s, j=0):
        at = pl.ds(*(got_tiles if u == last else whole)[j])
        index = u * PIECES + spans.index(s) if u < last else (
            last * PIECES + last_spans.index(s) * len(got_tiles) + j
        )
        return pltpu.make_async_remote_copy(
            src_ref=y_out.at[u, piece_at(s), at], dst_ref=y_got.at[u, piece_at(s), at],
            send_sem=y_send, recv_sem=y_recv.at[index],
            device_id=y_peer, device_id_type=MESH,
        )

    def z_copy(u, s, j=0, slot=None):
        at = pl.ds(*(got_tiles if u == 2 else whole)[j])
        goal, into, index = beside, u, last * PIECES + j
        if u < 2:
            goal = inner * target_z(u) + (1 - inner) * beside
            into = inner * last + (1 - inner) * u
            into = into if slot is None else slot
            index = (inner * 2 + (1 - inner) * u if slot is None else min(slot, 2)) * PIECES
            index = index + spans.index(s)
        else:
            index += last_spans.index(s) * len(got_tiles)
        return pltpu.make_async_remote_copy(
            src_ref=z_out.at[u, piece_at(s), at], dst_ref=z_got.at[into, piece_at(s), at],
            send_sem=z_send, recv_sem=z_recv.at[index],
            device_id=on_z(goal), device_id_type=MESH,
        )

    def peak_copy(buffer, i, partner, at):
        return pltpu.make_async_remote_copy(
            src_ref=buffer.at[0], dst_ref=buffer.at[i],
            send_sem=pk_send, recv_sem=pk_recv.at[at],
            device_id=partner, device_id_type=MESH,
        )

    core_peak = peak_copy(core_peaks, 1, sibling, 0)
    y_peak = peak_copy(y_peaks, 1, y_peer, 1)
    near_peak = peak_copy(near_peaks, 1, z_near, 2)
    far_peak = peak_copy(far_peaks, 1, z_far, 3)

    def act_peak_copy(t):
        return pltpu.make_async_remote_copy(
            src_ref=act_peaks.at[0], dst_ref=act_peaks.at[t],
            send_sem=ap_send.at[t - 1], recv_sem=ap_recv.at[t - 1],
            device_id=on_tensor(t), device_id_type=MESH,
        )

    def turn_act(u, k):
        at = pair_cols(u, k)
        read = act_own[:, at]
        top = jnp.max(jnp.abs(read).reshape(tokens // SUBLANES, SUBLANES, CORES * block), axis=0)
        core_peaks[0, :, at] = jnp.max(top.astype(jnp.float32), axis=0, keepdims=True)
        act_down[pair_at(u, k)] = jnp.transpose(read).reshape(CORES, block, tokens)

    def send_x(group, cuts):
        for cut in range(cuts):
            for u, k, s in group:
                for t in range(1, tensor):
                    x_copy(t, u, k, s, cut, cuts).start()

    act_load(0, 0).wait()
    turn_act(0, 0)
    pl.semaphore_wait(barrier, len(partners) + below + above)
    greet(far_sem)
    smalls[1].wait()
    act_tops[0] = jnp.max(act_hist[0], axis=0, keepdims=True)
    for t in range(1, tensor):
        top_copy(t).start()
    turned = {(0, 0)}
    for i, group in enumerate(order):
        for u, k, s in group:
            if (u, k) not in turned:
                if len(turned) == 1:
                    act_rest().wait()
                turn_act(u, k)
                turned.add((u, k))
        send_x(group, cuts_at[i])
        if i == 1:
            for t in range(1, tensor):
                hist_copy(t, 0).start()

    smalls[0].wait()
    if padded > cols:
        grad_scale[:, padded - LANES:] = jnp.ones((1, LANES), jnp.float32)
    grad_scale[:, :cols] = QUANT_LIMIT / jnp.maximum(
        jnp.max(grad_hist[...], axis=0, keepdims=True), SCALE_FLOOR
    )

    def quantize_cols(j):
        at = pl.ds(pl.multiple_of(j * LANES, LANES), LANES)
        scale = grad_scale[:, at]
        top = jnp.zeros((SUBLANES, LANES), jnp.bfloat16)
        for start, size in tiles(rows, TURN):
            turned = jnp.transpose(raw[at, start:start + size])
            mag = jnp.abs(turned).reshape(size // SUBLANES, SUBLANES, LANES)
            top = jnp.maximum(top, jnp.max(mag, axis=0))
            gq[start:start + size, at] = quantize(turned, scale)
        here = pl.ds(pl.multiple_of(width + j * LANES, LANES), LANES)
        core_peaks[0, :, here] = jnp.max(top.astype(jnp.float32), axis=0, keepdims=True)

    def grad_chunk(i, carry):
        grad_load(i).wait()
        for j in range(GROUP):
            quantize_cols(i * GROUP + j)
        return carry

    lax.fori_loop(0, groups, grad_chunk, 0)
    if rest:
        grad_load(groups, rest).wait()
        for j in range(pl.cdiv(rest, LANES)):
            quantize_cols(groups * GROUP + j)
    core_peak.start()
    pl.semaphore_wait(far_sem, below + above)

    smalls[2].wait()
    owner = owner_ref[...]
    top = act_tops[0]
    for t in range(1, tensor):
        top_copy(t).wait()
        top = jnp.where(owner == lax.rem(mt + tensor - t, tensor), act_tops[t], top)
    act_scale[...] = QUANT_LIMIT / jnp.maximum(top, SCALE_FLOOR)
    for start in range(0, width, LANES):
        turned = jnp.transpose(jnp.broadcast_to(act_scale[:, start:start + LANES], (LANES, LANES)))
        first = start // block
        scale_down[first:first + LANES // block] = turned.reshape(LANES // block, block, LANES)

    def load_own(u):
        at = pl.ds(target_z(u) * (ROWS_Y * CORES), ROWS_Y * CORES)
        count = ROWS_Y * CORES * block
        scale = scale_down[at].reshape(count, LANES)
        for start in range(0, tokens, LANES):
            read = act_down[at, :, start:start + LANES].reshape(count, LANES)
            own_lhs[:, start:start + LANES] = quantize(read, scale)

    def own_product(u, j):
        start, size = own_tiles[j]
        source = pl.ds(pl.multiple_of(mt * tokens, tokens), tokens)
        part[u, :, start:start + size] = jnp.dot(
            own_lhs[...], gq[source, start:start + size], preferred_element_type=jnp.float32
        )

    def got_product(group, cuts):
        span = tokens // cuts
        places, total = [], 0
        for u, k, s in group:
            places.append((u, k, s, total))
            total += CORES * s[1]
        for cut in range(cuts):
            first = cut * span
            for u, k, s, base in places:
                count = CORES * s[1]
                scale = scale_down[pair_at(u, k), piece_at(s), :].reshape(count, LANES)
                for t in range(1, tensor):
                    x_copy(t, u, k, s, cut, cuts).wait_recv()
                    for start in range(first, first + span, LANES):
                        read = act_got[t - 1, pair_at(u, k), piece_at(s), start:start + LANES]
                        got_lhs[t - 1, base:base + count, start:start + LANES] = quantize(
                            read.reshape(count, LANES), scale
                        )
            for j, (start, size) in enumerate(got_tiles):
                for t in range(1, tensor):
                    from_rank = lax.rem(mt + tensor - t, tensor)
                    source = pl.ds(pl.multiple_of(from_rank * tokens + first, TURN), span)
                    term = jnp.dot(
                        got_lhs[t - 1, :total, first:first + span],
                        gq[source, start:start + size], preferred_element_type=jnp.float32,
                    )
                    for u, k, s, base in places:
                        for c in range(CORES):
                            at = base + c * s[1]
                            part[u, part_rows(k, c, s), start:start + size] += term[at:at + s[1]]
                if cut == cuts - 1:
                    for u, k, s in group:
                        core_copy(u, k, s, j).start()

    def core_sum(u, k, s, j):
        start, size = got_tiles[j]
        core_copy(u, k, s, j).wait_recv()
        return (
            part[u, part_rows(k, core, s), start:start + size]
            + core_got[number[u, k, s], :s[1], start:start + size]
        )

    def send_y(u, s, j):
        start, size = got_tiles[j]
        y_out[u, piece_at(s), start:start + size] = core_sum(u, 0, s, j).astype(jnp.bfloat16)
        if u == last or j == len(got_tiles) - 1:
            y_copy(u, s, j if u == last else 0).start()

    def line_sum(u, s, j):
        start, size = got_tiles[j]
        return core_sum(u, 1, s, j) + y_got[u, piece_at(s), start:start + size].astype(jnp.float32)

    def send_z(u, s, add, j):
        start, size = got_tiles[j]
        if j == 0 and (u < last - 1 or s != cut_spans[1]):
            y_copy(u, spans[s[0] // piece]).wait_recv()
        if j == 0 and add:
            z_copy(u, s, 0, u).wait_recv()
        total = line_sum(u, s, j)
        if add:
            total = total + z_got[u, piece_at(s), start:start + size].astype(jnp.float32)
        z_out[u, piece_at(s), start:start + size] = total.astype(jnp.bfloat16)
        if u == 2 or j == len(got_tiles) - 1:
            z_copy(u, s, j if u == 2 else 0).start()

    load_own(0)
    for j in range(len(own_tiles)):
        own_product(0, j)
    core_peak.wait()
    y_peaks[0] = jnp.max(core_peaks[...], axis=0)
    y_peak.start()

    def finish_line(s):
        z_copy(0, s, 0, last).wait_recv()
        for j, (start, size) in enumerate(got_tiles):
            for part_of in last_spans:
                if s[0] <= part_of[0] < s[0] + s[1]:
                    z_copy(last - 1, part_of, j).wait_recv()
                    y_copy(last, part_of, j).wait_recv()
            total = line_sum(last, s, j)
            for u in (2, last):
                total = total + z_got[u, piece_at(s), start:start + size].astype(jnp.float32)
            total = total * undo[s[0]:s[0] + s[1], :1]
            total = total * grad_undo[:, start:start + size]
            size = min(size, cols - start)
            weight_ref[piece_at(s), start:start + size] = total[:, :size]

    where = {step: i for i, group in enumerate(order) for step in group}
    fillers, sends = [[] for _ in order], [[] for _ in order]
    far_sends = [[], []]
    for u, k, s in number:
        i = where[u, k, s]
        if k == 0:
            sends[i + (1 if u == 0 else 0)].append((0, u, s))
        elif u < 2:
            far_sends[0].append((i + 2 - u, u, s))
            far_sends[1].append((i + 5 - 2 * u, u, s))
        elif u == 2:
            sends[i if s in cut_spans else i + 1].append((1, u, s))
    starts = [where[u, 0, spans[0]] for u in range(depth)]
    for u in range(last):
        for j in range(len(own_tiles)):
            fillers[min(starts[u] + j, starts[u + 1] - 1)].append((u + 1, j))
    for i, group in enumerate(order):
        got_product(group, cuts_at[i])
        if i in starts[:last]:
            load_own(starts.index(i) + 1)
        for other, j in fillers[i]:
            own_product(other, j)
        for add, plan in enumerate(far_sends):
            due = [(other, piece_of) for at, other, piece_of in plan if at == i]

            @pl.when(inner == add)
            def _(due=due, add=add):
                for other, piece_of in due:
                    for j in range(len(got_tiles)):
                        send_z(other, piece_of, add, j)

        for j in range(len(got_tiles)):
            for kind, other, piece_of in sends[i]:
                if kind == 0:
                    send_y(other, piece_of, j)
                else:
                    send_z(other, piece_of, 0, j)
        if i == steps - 1:
            y_peak.wait()
            near_peaks[0] = jnp.max(y_peaks[...], axis=0)
            near_peak.start()
            pass_hist(1)
        if i == steps + 1:
            near_peak.wait()
            far_peaks[0] = jnp.max(near_peaks[...], axis=0)
            far_peak.start()
            pass_hist(2)
        if i == where[last, 0, cut_spans[1]]:
            far_peak.wait()
            tops = jnp.max(far_peaks[...], axis=0)
            act_peaks[0] = tops[:, :width]
            for t in range(1, tensor):
                act_peak_copy(t).start()
            factor = 1.0 / math.sqrt(rows * dp)
            grad_undo[...] = factor / grad_scale[...]
            undo = 1.0 / scale_down[me]
            pass_hist(3)
            smalls[3].wait()
            slots = slot_ref[...]
            hist_row = lax.broadcasted_iota(jnp.int32, grad_hist.shape, 0)
            grad_slots = slots[width:width + cols]
            for t in range(1, tensor):
                first = width + t * cols
                grad_slots = jnp.where(mt == t, slots[first:first + cols], grad_slots)
            grad_hist_out[...] = jnp.where(
                hist_row == grad_slots[None, :], tops[:, width:width + cols], grad_hist[...]
            )
        if i == len(order) - 1:
            for t in range(1, tensor):
                act_peak_copy(t).wait()
            current = act_hist[0]
            for t in range(1, tensor):
                source = lax.rem(mt + tensor - t, tensor)
                current = jnp.where(owner_ref[...] == source, hist_got[t - 1], current)
            hist_row = lax.broadcasted_iota(jnp.int32, current.shape, 0)
            act_hist_out[0] = jnp.where(
                hist_row == slots[:width][None, :], jnp.max(act_peaks[...], axis=0), current
            )
            for span in spans:
                finish_line(span)

    def all_sent(held, semaphore):
        pltpu.make_async_remote_copy(
            src_ref=held, dst_ref=held, send_sem=semaphore, recv_sem=semaphore,
            device_id=sibling, device_id_type=MESH,
        ).wait_send()

    for t in range(1, tensor):
        all_sent(act_down, x_send.at[t - 1])
    all_sent(part.at[pl.ds(0, depth // CORES)], core_send)
    all_sent(y_out, y_send)
    all_sent(z_out, z_send)


def fused_outputs(activations, gradients, act_history, grad_history, owner_rank, history_slot):
    dp, tensor = lax.axis_size("dp"), lax.axis_size("tensor")
    tokens, width = activations.shape
    rows, cols = gradients.shape
    hist = act_history.shape[1]
    depth = dp // (CORES * ROWS_Y)
    blocks, block = dp, width // dp
    order = piece_plan(block)[2]
    steps = sum(len(group) for group in order)
    slots, cuts_at = x_plan(order)
    pieces = max(slots.values()) + cuts_at[-1]
    hops = (depth - 1) * PIECES + (PIECES + 1) * len(tiles(pl.cdiv(cols, LANES) * LANES, GOT_TILE))
    padded = pl.cdiv(cols, LANES) * LANES
    line = ROWS_Y * CORES * block
    dma = pltpu.SemaphoreType.DMA
    vmem = pl.BlockSpec(memory_space=pltpu.VMEM)
    hbm = pl.BlockSpec(memory_space=pl.ANY)
    f32, bf16, i32 = jnp.float32, jnp.bfloat16, jnp.int32
    others = tensor - 1
    halves = len(tiles(padded, GOT_TILE))
    loads = pl.cdiv(cols, GROUP * LANES)
    return pl.pallas_call(
        functools.partial(fused_kernel, dp, tensor),
        out_shape=(
            pltpu.VMEM((block, cols), f32),
            pltpu.VMEM((1, hist, width), f32),
            pltpu.VMEM((hist, cols), f32),
        ),
        in_specs=[hbm] * 6,
        out_specs=(vmem, vmem, vmem),
        scratch_shapes=[
            pltpu.VMEM((tokens, width), bf16),
            pltpu.VMEM((blocks, block, tokens), bf16),
            pltpu.VMEM((others, blocks, block, tokens), bf16),
            pltpu.VMEM((padded, rows), bf16),
            pltpu.VMEM((rows, padded), bf16),
            pltpu.VMEM((depth, line, padded), f32),
            pltpu.VMEM((steps, block // PIECES, padded), f32),
            pltpu.VMEM((depth, block, padded), bf16),
            pltpu.VMEM((depth, block, padded), bf16),
            pltpu.VMEM((depth - 1, block, padded), bf16),
            pltpu.VMEM((depth, block, padded), bf16),
            pltpu.VMEM((line, tokens), bf16),
            pltpu.VMEM((others, CORES * (block // PIECES), tokens), bf16),
            pltpu.VMEM((1, hist, width), f32),
            pltpu.VMEM((others, hist, width), f32),
            pltpu.VMEM((hist, cols), f32),
            pltpu.VMEM((1, width), i32),
            pltpu.VMEM(history_slot.shape, i32),
            pltpu.VMEM((2, 1, width + padded), f32),
            pltpu.VMEM((2, 1, width + padded), f32),
            pltpu.VMEM((2, 1, width + padded), f32),
            pltpu.VMEM((2, 1, width + padded), f32),
            pltpu.VMEM((tensor, 1, width), f32),
            pltpu.VMEM((tensor, 1, width), f32),
            pltpu.VMEM((1, width), f32),
            pltpu.VMEM((blocks, block, LANES), f32),
            pltpu.VMEM((1, padded), f32),
            pltpu.VMEM((1, padded), f32),
            pltpu.SemaphoreType.REGULAR,
            dma((2,)), dma((loads,)), dma((4,)),
            dma((others,)), dma((others, 3)), dma((others,)), dma((others,)),
            dma((others,)), dma((others, pieces)), dma, dma((RING, halves)),
            dma, dma((hops,)), dma, dma((hops,)),
            dma, dma((4,)), dma((others,)), dma((others,)),
        ],
        compiler_params=pltpu.CompilerParams(
            collective_id=0, has_side_effects=True, vmem_limit_bytes=61 * 1024 * 1024
        ),
    )(
        activations, gradients.T, act_history, grad_history,
        owner_rank[None, :], history_slot,
    )


def hand_over_kernel(*refs):
    sems = refs[-1]
    half = (len(refs) - 1) // 2
    copies = [
        pltpu.make_async_copy(source, target, sems.at[i])
        for i, (source, target) in enumerate(zip(refs[:half], refs[half:-1]))
    ]
    for copy in copies:
        copy.start()
    for copy in copies:
        copy.wait()


def hand_over(*results):
    vmem = pl.BlockSpec(memory_space=pltpu.VMEM)
    hbm = pl.BlockSpec(memory_space=pl.ANY)
    return pl.pallas_call(
        hand_over_kernel,
        out_shape=tuple(jax.ShapeDtypeStruct(r.shape, r.dtype) for r in results),
        in_specs=[vmem] * len(results),
        out_specs=(hbm,) * len(results),
        scratch_shapes=[pltpu.SemaphoreType.DMA((len(results),))],
        compiler_params=pltpu.CompilerParams(vmem_limit_bytes=1024 * 1024),
    )(*results)


def gathered_sums(activations, gradients, act_history, grad_history, owner_rank):
    my_rank = lax.axis_index("tensor")
    held = jnp.where(owner_rank[None, :] == my_rank, act_history[0], jnp.float32(0.0))
    current = lax.psum(held, "tensor")
    act_scale = QUANT_LIMIT / jnp.maximum(jnp.max(current, axis=0), SCALE_FLOOR)
    grad_scale = QUANT_LIMIT / jnp.maximum(jnp.max(grad_history, axis=0), SCALE_FLOOR)
    gathered_rows = lax.all_gather(quantize(activations, act_scale), "tensor", axis=0, tiled=True)
    summed = lax.psum_scatter(
        lax.dot_general(
            gathered_rows, quantize(gradients, grad_scale), (((0,), (0,)), ((), ())),
            preferred_element_type=jnp.float32,
        ),
        "dp", scatter_dimension=0, tiled=True,
    )
    act_peak = lax.pmax(jnp.max(jnp.abs(activations), axis=0).astype(jnp.float32), ("dp", "tensor"))
    grad_peak = lax.pmax(jnp.max(jnp.abs(gradients), axis=0).astype(jnp.float32), "dp")
    return summed, current, act_peak[None, :], grad_peak[None, :]


def body(activations, gradients, act_history, grad_history, owner_rank, history_slot):
    dp = lax.axis_size("dp")
    model_width = act_history.shape[2]
    column_total = gradients.shape[1]
    row_count = model_width // dp
    fits = dp == CORES * ROWS_Y * DEPTH
    fits = fits and (row_count * CORES) % LANES == 0 and row_count % (PIECES * 2 * SUBLANES) == 0
    fits = fits and model_width % (CORES * ROWS_Y * LANES) == 0 and activations.shape[0] % (TAIL_CUTS * TURN) == 0
    fits = fits and column_total % SUBLANES == 0
    if fits:
        return hand_over(*fused_outputs(
            activations, gradients, act_history, grad_history, owner_rank, history_slot
        ))
    act_slots = history_slot[:model_width]
    grad_slots = lax.dynamic_slice_in_dim(
        history_slot, model_width + lax.axis_index("tensor") * column_total, column_total, 0
    )
    summed, current, act_peak, grad_peak = gathered_sums(
        activations, gradients, act_history, grad_history, owner_rank
    )
    act_scale = QUANT_LIMIT / jnp.maximum(jnp.max(current, axis=0), SCALE_FLOOR)
    grad_scale = QUANT_LIMIT / jnp.maximum(jnp.max(grad_history, axis=0), SCALE_FLOOR)
    grad_factor = 1.0 / math.sqrt(gradients.shape[0] * dp)
    row_base = lax.axis_index("dp") * row_count
    row_scale = lax.dynamic_slice_in_dim(act_scale, row_base, row_count, 0)
    weight_grad = summed / (row_scale[:, None] * grad_scale[None, :]) * grad_factor
    act_history_out = place_peaks(current, act_peak[0], act_slots)[None]
    grad_history_out = place_peaks(grad_history, grad_peak[0], grad_slots)
    return (weight_grad, act_history_out, grad_history_out)


def solution(mesh):
    placed = (
        P(("dp", "tensor"), None),
        P("dp", "tensor"),
        P("tensor", None, None),
        P(None, "tensor"),
        P(),
        P(),
    )
    return jax.shard_map(
        body,
        mesh=mesh,
        in_specs=placed,
        out_specs=(P("dp", "tensor"), P("tensor", None, None), P(None, "tensor")),
        check_vma=False,
    )
```

```python
import functools
import math

import jax
import jax.numpy as jnp
from jax import lax
from jax.experimental import pallas as pl
from jax.experimental.pallas import tpu as pltpu
from jax.sharding import PartitionSpec as P

QUANT_LIMIT = 448.0
SCALE_FLOOR = 0.25
CORES = 2
ROWS_Y = 2
DEPTH = 4
LANES = 128
SUBLANES = 16
PIECES = 2
OWN_TILE = 768
GOT_TILE = 1536
TAIL_CUTS = 2
TAIL_STEPS = 1
RING = 8
GROUP = 3
TURN = 256
MESH = pl.DeviceIdType.MESH


def quantize(values, scale):
    scaled = values.astype(jnp.float32) * scale
    return jnp.clip(scaled, -QUANT_LIMIT, QUANT_LIMIT).astype(jnp.bfloat16)


def place_peaks(history, peaks, slots):
    rows = lax.broadcasted_iota(jnp.int32, history.shape, 0)
    return jnp.where(rows == slots[None, :], peaks[None, :], history)


def tiles(width, step):
    return [(start, min(step, width - start)) for start in range(0, width, step)]


def piece_plan(block):
    size = block // PIECES
    fine = size // 2
    spans = [(i * size, size) for i in range(PIECES)]
    order = [[(u, k, s)] for u in range(DEPTH) for k in range(ROWS_Y) for s in spans]
    last = DEPTH - 1
    at = order.index([(last, 0, spans[0])])
    cuts = [(block - size + i * fine, fine) for i in range(2)]
    order[at - 1] = order[at]
    order[at:at + 2] = [[(last, 0, cut), (last - 1, 1, cut)] for cut in cuts]
    order[at + 2:] = [[(last, 1, s) for s in spans]]
    return spans, cuts, order


def x_plan(order):
    slots, cuts_at, free = {}, [], 0
    for i, group in enumerate(order):
        cuts_at.append(TAIL_CUTS if i >= len(order) - TAIL_STEPS else 1)
        for step in group:
            slots[step] = free
            free += cuts_at[-1]
    return slots, cuts_at


def fused_kernel(
    dp, tensor,
    act_hbm, grad_hbm, act_hist_hbm, grad_hist_hbm, owner_hbm, slot_hbm,
    weight_ref, act_hist_out, grad_hist_out,
    act_own, act_down, act_got, raw, gq, part, core_got, y_out, y_got, z_out, z_got,
    own_lhs, got_lhs, act_hist, hist_got, grad_hist, owner_ref, slot_ref,
    core_peaks, y_peaks, near_peaks, far_peaks, act_peaks,
    act_tops, act_scale, scale_down, grad_scale, grad_undo, far_sem,
    load_sem, grad_sem, small_sem, hist_send, hist_recv, top_send, top_recv,
    x_send, x_recv, core_send, core_recv, y_send, y_recv, z_send, z_recv,
    pk_send, pk_recv, ap_send, ap_recv,
):
    me = lax.axis_index("dp")
    mt = lax.axis_index("tensor")
    core = lax.rem(me, CORES)
    chip = lax.div(me, CORES)
    yy = lax.rem(chip, ROWS_Y)
    zz = lax.div(chip, ROWS_Y)
    depth = DEPTH
    half, odd = lax.div(zz, 2), lax.rem(zz, 2)
    inner = odd * (1 - half) + (1 - odd) * half
    beside = 2 * half + 1 - odd
    tokens, width = act_hbm.shape
    cols, rows = grad_hbm.shape
    block = width // dp
    piece = block // PIECES
    padded = grad_scale.shape[1]
    own_tiles = tiles(padded, OWN_TILE)
    got_tiles = tiles(padded, GOT_TILE)
    steps = ROWS_Y * PIECES
    last = depth - 1
    spans, cut_spans, order = piece_plan(block)
    number = {step: i for i, step in enumerate(step for group in order for step in group)}
    last_spans = spans[:-1] + cut_spans
    x_slots, cuts_at = x_plan(order)

    def dp_index(z, y, c):
        return (z * ROWS_Y + y) * CORES + c

    def on_tensor(t):
        return {"tensor": lax.rem(mt + t, tensor)}

    sibling = {"dp": dp_index(zz, yy, 1 - core)}
    y_peer = {"dp": dp_index(zz, 1 - yy, core)}

    def on_z(z):
        return {"dp": dp_index(z, yy, core)}

    z_near, z_far = on_z(beside), on_z(2 * (1 - half) + odd)

    barrier = pltpu.get_barrier_semaphore()
    partners = [on_tensor(t) for t in range(1, tensor)] + [sibling, y_peer]
    below = lax.div(zz + depth - 1, depth)
    above = 1 - lax.div(zz + 1, depth)

    def greet(semaphore):
        @pl.when(zz > 0)
        def _():
            pl.semaphore_signal(semaphore, inc=1, device_id=on_z(zz - 1), device_id_type=MESH)

        @pl.when(zz < depth - 1)
        def _():
            pl.semaphore_signal(semaphore, inc=1, device_id=on_z(zz + 1), device_id_type=MESH)

    for partner in partners:
        pl.semaphore_signal(barrier, inc=1, device_id=partner, device_id_type=MESH)
    greet(barrier)

    def target_z(u):
        return (3 * (1 - half), 2 - half, beside, zz)[u]

    def side(k):
        return yy * k + (1 - yy) * (1 - k)

    def pair_of(u, k):
        return target_z(u) * ROWS_Y + side(k)

    def pair_at(u, k):
        return pl.ds(pair_of(u, k) * CORES, CORES)

    def pair_cols(u, k):
        return pl.ds(pl.multiple_of(pair_of(u, k) * (CORES * block), LANES), CORES * block)

    def act_load(u, k):
        at = pair_cols(u, k)
        return pltpu.make_async_copy(
            act_hbm.at[:, at], act_own.at[:, at], load_sem.at[min(u * ROWS_Y + k, 1)]
        )

    def act_rest():
        at = pl.ds(0, width - CORES * block)
        return pltpu.make_async_copy(act_hbm.at[:, at], act_own.at[:, at], load_sem.at[1])

    for u in range(depth):
        for k in range(ROWS_Y):
            act_load(u, k).start()
    smalls = [
        pltpu.make_async_copy(source, target, small_sem.at[i])
        for i, (source, target) in enumerate((
            (grad_hist_hbm, grad_hist), (act_hist_hbm, act_hist),
            (owner_hbm, owner_ref), (slot_hbm, slot_ref),
        ))
    ]
    for small in smalls:
        small.start()

    wide = GROUP * LANES
    groups, rest = cols // wide, cols % wide

    def grad_load(i, size=wide):
        at = pl.ds(i * wide, size)
        return pltpu.make_async_copy(grad_hbm.at[at], raw.at[at], grad_sem.at[i])

    def start_load(i, carry):
        grad_load(i).start()
        return carry

    lax.fori_loop(0, groups, start_load, 0)
    if rest:
        grad_load(groups, rest).start()
    if padded > cols:
        raw[cols:, :] = jnp.zeros((padded - cols, rows), jnp.bfloat16)

    def piece_at(s):
        return pl.ds(*s)

    def part_rows(k, c, s):
        return pl.ds(pl.multiple_of((side(k) * CORES + c) * block + s[0], s[1]), s[1])

    def hist_copy(t, stage):
        parts = CORES if stage == 2 else CORES * ROWS_Y
        mine = core if stage == 2 else core * ROWS_Y + yy
        at = pl.ds(pl.multiple_of(mine * (width // parts), LANES), width // parts)
        held = hist_got.at[t - 1, :, at]
        return pltpu.make_async_remote_copy(
            src_ref=held if stage else act_hist_hbm.at[0, :, at], dst_ref=held,
            send_sem=hist_send.at[t - 1], recv_sem=hist_recv.at[t - 1, stage],
            device_id=(on_tensor(t), y_peer, sibling)[stage], device_id_type=MESH,
        )

    def top_copy(t):
        return pltpu.make_async_remote_copy(
            src_ref=act_tops.at[0], dst_ref=act_tops.at[t],
            send_sem=top_send.at[t - 1], recv_sem=top_recv.at[t - 1],
            device_id=on_tensor(t), device_id_type=MESH,
        )

    def pass_hist(stage):
        for t in range(1, tensor):
            hist_copy(t, stage - 1).wait()
            if stage < 3:
                hist_copy(t, stage).start()

    def x_copy(t, u, k, s, cut=0, cuts=1):
        at = x_slots[u, k, s] + cut
        span = pl.ds(cut * (tokens // cuts), tokens // cuts)
        return pltpu.make_async_remote_copy(
            src_ref=act_down.at[pair_at(u, k), piece_at(s), span],
            dst_ref=act_got.at[t - 1, pair_at(u, k), piece_at(s), span],
            send_sem=x_send.at[t - 1], recv_sem=x_recv.at[t - 1, at],
            device_id=on_tensor(t), device_id_type=MESH,
        )

    def core_copy(u, k, s, j):
        at = number[u, k, s]
        start, size = got_tiles[j]
        return pltpu.make_async_remote_copy(
            src_ref=part.at[u, part_rows(k, 1 - core, s), pl.ds(start, size)],
            dst_ref=core_got.at[at, pl.ds(0, s[1]), pl.ds(start, size)],
            send_sem=core_send, recv_sem=core_recv.at[at % RING, j],
            device_id=sibling, device_id_type=MESH,
        )

    whole = [(0, padded)]

    def y_copy(u, s, j=0):
        at = pl.ds(*(got_tiles if u == last else whole)[j])
        index = u * PIECES + spans.index(s) if u < last else (
            last * PIECES + last_spans.index(s) * len(got_tiles) + j
        )
        return pltpu.make_async_remote_copy(
            src_ref=y_out.at[u, piece_at(s), at], dst_ref=y_got.at[u, piece_at(s), at],
            send_sem=y_send, recv_sem=y_recv.at[index],
            device_id=y_peer, device_id_type=MESH,
        )

    def z_copy(u, s, j=0, slot=None):
        at = pl.ds(*(got_tiles if u == 2 else whole)[j])
        goal, into, index = beside, u, last * PIECES + j
        if u < 2:
            goal = inner * target_z(u) + (1 - inner) * beside
            into = inner * last + (1 - inner) * u
            into = into if slot is None else slot
            index = (inner * 2 + (1 - inner) * u if slot is None else min(slot, 2)) * PIECES
            index = index + spans.index(s)
        else:
            index += last_spans.index(s) * len(got_tiles)
        return pltpu.make_async_remote_copy(
            src_ref=z_out.at[u, piece_at(s), at], dst_ref=z_got.at[into, piece_at(s), at],
            send_sem=z_send, recv_sem=z_recv.at[index],
            device_id=on_z(goal), device_id_type=MESH,
        )

    def peak_copy(buffer, i, partner, at):
        return pltpu.make_async_remote_copy(
            src_ref=buffer.at[0], dst_ref=buffer.at[i],
            send_sem=pk_send, recv_sem=pk_recv.at[at],
            device_id=partner, device_id_type=MESH,
        )

    core_peak = peak_copy(core_peaks, 1, sibling, 0)
    y_peak = peak_copy(y_peaks, 1, y_peer, 1)
    near_peak = peak_copy(near_peaks, 1, z_near, 2)
    far_peak = peak_copy(far_peaks, 1, z_far, 3)

    def act_peak_copy(t):
        return pltpu.make_async_remote_copy(
            src_ref=act_peaks.at[0], dst_ref=act_peaks.at[t],
            send_sem=ap_send.at[t - 1], recv_sem=ap_recv.at[t - 1],
            device_id=on_tensor(t), device_id_type=MESH,
        )

    def turn_act(u, k):
        at = pair_cols(u, k)
        read = act_own[:, at]
        top = jnp.max(jnp.abs(read).reshape(tokens // SUBLANES, SUBLANES, CORES * block), axis=0)
        core_peaks[0, :, at] = jnp.max(top.astype(jnp.float32), axis=0, keepdims=True)
        act_down[pair_at(u, k)] = jnp.transpose(read).reshape(CORES, block, tokens)

    def send_x(group, cuts):
        for cut in range(cuts):
            for u, k, s in group:
                for t in range(1, tensor):
                    x_copy(t, u, k, s, cut, cuts).start()

    act_load(0, 0).wait()
    turn_act(0, 0)
    pl.semaphore_wait(barrier, len(partners) + below + above)
    greet(far_sem)
    smalls[1].wait()
    act_tops[0] = jnp.max(act_hist[0], axis=0, keepdims=True)
    for t in range(1, tensor):
        top_copy(t).start()
    turned = {(0, 0)}
    for i, group in enumerate(order):
        for u, k, s in group:
            if (u, k) not in turned:
                if len(turned) == 1:
                    act_rest().wait()
                turn_act(u, k)
                turned.add((u, k))
        send_x(group, cuts_at[i])
        if i == 1:
            for t in range(1, tensor):
                hist_copy(t, 0).start()

    smalls[0].wait()
    if padded > cols:
        grad_scale[:, padded - LANES:] = jnp.ones((1, LANES), jnp.float32)
    grad_scale[:, :cols] = QUANT_LIMIT / jnp.maximum(
        jnp.max(grad_hist[...], axis=0, keepdims=True), SCALE_FLOOR
    )

    def quantize_cols(j):
        at = pl.ds(pl.multiple_of(j * LANES, LANES), LANES)
        scale = grad_scale[:, at]
        top = jnp.zeros((SUBLANES, LANES), jnp.bfloat16)
        for start, size in tiles(rows, TURN):
            turned = jnp.transpose(raw[at, start:start + size])
            mag = jnp.abs(turned).reshape(size // SUBLANES, SUBLANES, LANES)
            top = jnp.maximum(top, jnp.max(mag, axis=0))
            gq[start:start + size, at] = quantize(turned, scale)
        here = pl.ds(pl.multiple_of(width + j * LANES, LANES), LANES)
        core_peaks[0, :, here] = jnp.max(top.astype(jnp.float32), axis=0, keepdims=True)

    def grad_chunk(i, carry):
        grad_load(i).wait()
        for j in range(GROUP):
            quantize_cols(i * GROUP + j)
        return carry

    lax.fori_loop(0, groups, grad_chunk, 0)
    if rest:
        grad_load(groups, rest).wait()
        for j in range(pl.cdiv(rest, LANES)):
            quantize_cols(groups * GROUP + j)
    core_peak.start()
    pl.semaphore_wait(far_sem, below + above)

    smalls[2].wait()
    owner = owner_ref[...]
    top = act_tops[0]
    for t in range(1, tensor):
        top_copy(t).wait()
        top = jnp.where(owner == lax.rem(mt + tensor - t, tensor), act_tops[t], top)
    act_scale[...] = QUANT_LIMIT / jnp.maximum(top, SCALE_FLOOR)
    for start in range(0, width, LANES):
        turned = jnp.transpose(jnp.broadcast_to(act_scale[:, start:start + LANES], (LANES, LANES)))
        first = start // block
        scale_down[first:first + LANES // block] = turned.reshape(LANES // block, block, LANES)

    def load_own(u):
        at = pl.ds(target_z(u) * (ROWS_Y * CORES), ROWS_Y * CORES)
        count = ROWS_Y * CORES * block
        scale = scale_down[at].reshape(count, LANES)
        for start in range(0, tokens, LANES):
            read = act_down[at, :, start:start + LANES].reshape(count, LANES)
            own_lhs[:, start:start + LANES] = quantize(read, scale)

    def own_product(u, j):
        start, size = own_tiles[j]
        source = pl.ds(pl.multiple_of(mt * tokens, tokens), tokens)
        part[u, :, start:start + size] = jnp.dot(
            own_lhs[...], gq[source, start:start + size], preferred_element_type=jnp.float32
        )

    def got_product(group, cuts):
        span = tokens // cuts
        places, total = [], 0
        for u, k, s in group:
            places.append((u, k, s, total))
            total += CORES * s[1]
        for cut in range(cuts):
            first = cut * span
            for u, k, s, base in places:
                count = CORES * s[1]
                scale = scale_down[pair_at(u, k), piece_at(s), :].reshape(count, LANES)
                for t in range(1, tensor):
                    x_copy(t, u, k, s, cut, cuts).wait_recv()
                    for start in range(first, first + span, LANES):
                        read = act_got[t - 1, pair_at(u, k), piece_at(s), start:start + LANES]
                        got_lhs[t - 1, base:base + count, start:start + LANES] = quantize(
                            read.reshape(count, LANES), scale
                        )
            for j, (start, size) in enumerate(got_tiles):
                for t in range(1, tensor):
                    from_rank = lax.rem(mt + tensor - t, tensor)
                    source = pl.ds(pl.multiple_of(from_rank * tokens + first, TURN), span)
                    term = jnp.dot(
                        got_lhs[t - 1, :total, first:first + span],
                        gq[source, start:start + size], preferred_element_type=jnp.float32,
                    )
                    for u, k, s, base in places:
                        for c in range(CORES):
                            at = base + c * s[1]
                            part[u, part_rows(k, c, s), start:start + size] += term[at:at + s[1]]
                if cut == cuts - 1:
                    for u, k, s in group:
                        core_copy(u, k, s, j).start()

    def core_sum(u, k, s, j):
        start, size = got_tiles[j]
        core_copy(u, k, s, j).wait_recv()
        return (
            part[u, part_rows(k, core, s), start:start + size]
            + core_got[number[u, k, s], :s[1], start:start + size]
        )

    def send_y(u, s, j):
        start, size = got_tiles[j]
        y_out[u, piece_at(s), start:start + size] = core_sum(u, 0, s, j).astype(jnp.bfloat16)
        if u == last or j == len(got_tiles) - 1:
            y_copy(u, s, j if u == last else 0).start()

    def line_sum(u, s, j):
        start, size = got_tiles[j]
        return core_sum(u, 1, s, j) + y_got[u, piece_at(s), start:start + size].astype(jnp.float32)

    def send_z(u, s, add, j):
        start, size = got_tiles[j]
        if j == 0 and (u < last - 1 or s != cut_spans[1]):
            y_copy(u, spans[s[0] // piece]).wait_recv()
        if j == 0 and add:
            z_copy(u, s, 0, u).wait_recv()
        total = line_sum(u, s, j)
        if add:
            total = total + z_got[u, piece_at(s), start:start + size].astype(jnp.float32)
        z_out[u, piece_at(s), start:start + size] = total.astype(jnp.bfloat16)
        if u == 2 or j == len(got_tiles) - 1:
            z_copy(u, s, j if u == 2 else 0).start()

    load_own(0)
    for j in range(len(own_tiles)):
        own_product(0, j)
    core_peak.wait()
    y_peaks[0] = jnp.max(core_peaks[...], axis=0)
    y_peak.start()

    def finish_line(s):
        z_copy(0, s, 0, last).wait_recv()
        for j, (start, size) in enumerate(got_tiles):
            for part_of in last_spans:
                if s[0] <= part_of[0] < s[0] + s[1]:
                    z_copy(last - 1, part_of, j).wait_recv()
                    y_copy(last, part_of, j).wait_recv()
            total = line_sum(last, s, j)
            for u in (2, last):
                total = total + z_got[u, piece_at(s), start:start + size].astype(jnp.float32)
            total = total * undo[s[0]:s[0] + s[1], :1]
            total = total * grad_undo[:, start:start + size]
            size = min(size, cols - start)
            weight_ref[piece_at(s), start:start + size] = total[:, :size]

    where = {step: i for i, group in enumerate(order) for step in group}
    fillers, sends = [[] for _ in order], [[] for _ in order]
    far_sends = [[], []]
    for u, k, s in number:
        i = where[u, k, s]
        if k == 0:
            sends[i + (1 if u == 0 else 0)].append((0, u, s))
        elif u < 2:
            far_sends[0].append((i + 2 - u, u, s))
            far_sends[1].append((i + 5 - 2 * u, u, s))
        elif u == 2:
            sends[i if s in cut_spans else i + 1].append((1, u, s))
    starts = [where[u, 0, spans[0]] for u in range(depth)]
    for u in range(last):
        for j in range(len(own_tiles)):
            fillers[min(starts[u] + j, starts[u + 1] - 1)].append((u + 1, j))
    for i, group in enumerate(order):
        got_product(group, cuts_at[i])
        if i in starts[:last]:
            load_own(starts.index(i) + 1)
        for other, j in fillers[i]:
            own_product(other, j)
        for add, plan in enumerate(far_sends):
            due = [(other, piece_of) for at, other, piece_of in plan if at == i]

            @pl.when(inner == add)
            def _(due=due, add=add):
                for other, piece_of in due:
                    for j in range(len(got_tiles)):
                        send_z(other, piece_of, add, j)

        for j in range(len(got_tiles)):
            for kind, other, piece_of in sends[i]:
                if kind == 0:
                    send_y(other, piece_of, j)
                else:
                    send_z(other, piece_of, 0, j)
        if i == steps - 1:
            y_peak.wait()
            near_peaks[0] = jnp.max(y_peaks[...], axis=0)
            near_peak.start()
            pass_hist(1)
        if i == steps + 1:
            near_peak.wait()
            far_peaks[0] = jnp.max(near_peaks[...], axis=0)
            far_peak.start()
            pass_hist(2)
        if i == where[last, 0, cut_spans[1]]:
            far_peak.wait()
            tops = jnp.max(far_peaks[...], axis=0)
            act_peaks[0] = tops[:, :width]
            for t in range(1, tensor):
                act_peak_copy(t).start()
            factor = 1.0 / math.sqrt(rows * dp)
            grad_undo[...] = factor / grad_scale[...]
            undo = 1.0 / scale_down[me]
            pass_hist(3)
            smalls[3].wait()
            slots = slot_ref[...]
            hist_row = lax.broadcasted_iota(jnp.int32, grad_hist.shape, 0)
            grad_slots = slots[width:width + cols]
            for t in range(1, tensor):
                first = width + t * cols
                grad_slots = jnp.where(mt == t, slots[first:first + cols], grad_slots)
            grad_hist_out[...] = jnp.where(
                hist_row == grad_slots[None, :], tops[:, width:width + cols], grad_hist[...]
            )
        if i == len(order) - 1:
            for t in range(1, tensor):
                act_peak_copy(t).wait()
            current = act_hist[0]
            for t in range(1, tensor):
                source = lax.rem(mt + tensor - t, tensor)
                current = jnp.where(owner_ref[...] == source, hist_got[t - 1], current)
            hist_row = lax.broadcasted_iota(jnp.int32, current.shape, 0)
            act_hist_out[0] = jnp.where(
                hist_row == slots[:width][None, :], jnp.max(act_peaks[...], axis=0), current
            )
            for span in spans:
                finish_line(span)

    def all_sent(held, semaphore):
        pltpu.make_async_remote_copy(
            src_ref=held, dst_ref=held, send_sem=semaphore, recv_sem=semaphore,
            device_id=sibling, device_id_type=MESH,
        ).wait_send()

    for t in range(1, tensor):
        all_sent(act_down, x_send.at[t - 1])
    all_sent(part.at[pl.ds(0, depth // CORES)], core_send)
    all_sent(y_out, y_send)
    all_sent(z_out, z_send)


def fused_outputs(activations, gradients, act_history, grad_history, owner_rank, history_slot):
    dp, tensor = lax.axis_size("dp"), lax.axis_size("tensor")
    tokens, width = activations.shape
    rows, cols = gradients.shape
    hist = act_history.shape[1]
    depth = dp // (CORES * ROWS_Y)
    blocks, block = dp, width // dp
    order = piece_plan(block)[2]
    steps = sum(len(group) for group in order)
    slots, cuts_at = x_plan(order)
    pieces = max(slots.values()) + cuts_at[-1]
    hops = (depth - 1) * PIECES + (PIECES + 1) * len(tiles(pl.cdiv(cols, LANES) * LANES, GOT_TILE))
    padded = pl.cdiv(cols, LANES) * LANES
    line = ROWS_Y * CORES * block
    dma = pltpu.SemaphoreType.DMA
    vmem = pl.BlockSpec(memory_space=pltpu.VMEM)
    hbm = pl.BlockSpec(memory_space=pl.ANY)
    f32, bf16, i32 = jnp.float32, jnp.bfloat16, jnp.int32
    others = tensor - 1
    halves = len(tiles(padded, GOT_TILE))
    loads = pl.cdiv(cols, GROUP * LANES)
    return pl.pallas_call(
        functools.partial(fused_kernel, dp, tensor),
        out_shape=(
            pltpu.VMEM((block, cols), f32),
            pltpu.VMEM((1, hist, width), f32),
            pltpu.VMEM((hist, cols), f32),
        ),
        in_specs=[hbm] * 6,
        out_specs=(vmem, vmem, vmem),
        scratch_shapes=[
            pltpu.VMEM((tokens, width), bf16),
            pltpu.VMEM((blocks, block, tokens), bf16),
            pltpu.VMEM((others, blocks, block, tokens), bf16),
            pltpu.VMEM((padded, rows), bf16),
            pltpu.VMEM((rows, padded), bf16),
            pltpu.VMEM((depth, line, padded), f32),
            pltpu.VMEM((steps, block // PIECES, padded), f32),
            pltpu.VMEM((depth, block, padded), bf16),
            pltpu.VMEM((depth, block, padded), bf16),
            pltpu.VMEM((depth - 1, block, padded), bf16),
            pltpu.VMEM((depth, block, padded), bf16),
            pltpu.VMEM((line, tokens), bf16),
            pltpu.VMEM((others, CORES * block, tokens), bf16),
            pltpu.VMEM((1, hist, width), f32),
            pltpu.VMEM((others, hist, width), f32),
            pltpu.VMEM((hist, cols), f32),
            pltpu.VMEM((1, width), i32),
            pltpu.VMEM(history_slot.shape, i32),
            pltpu.VMEM((2, 1, width + padded), f32),
            pltpu.VMEM((2, 1, width + padded), f32),
            pltpu.VMEM((2, 1, width + padded), f32),
            pltpu.VMEM((2, 1, width + padded), f32),
            pltpu.VMEM((tensor, 1, width), f32),
            pltpu.VMEM((tensor, 1, width), f32),
            pltpu.VMEM((1, width), f32),
            pltpu.VMEM((blocks, block, LANES), f32),
            pltpu.VMEM((1, padded), f32),
            pltpu.VMEM((1, padded), f32),
            pltpu.SemaphoreType.REGULAR,
            dma((2,)), dma((loads,)), dma((4,)),
            dma((others,)), dma((others, 3)), dma((others,)), dma((others,)),
            dma((others,)), dma((others, pieces)), dma, dma((RING, halves)),
            dma, dma((hops,)), dma, dma((hops,)),
            dma, dma((4,)), dma((others,)), dma((others,)),
        ],
        compiler_params=pltpu.CompilerParams(
            collective_id=0, has_side_effects=True, vmem_limit_bytes=61 * 1024 * 1024
        ),
    )(
        activations, gradients.T, act_history, grad_history,
        owner_rank[None, :], history_slot,
    )


def hand_over_kernel(*refs):
    sems = refs[-1]
    half = (len(refs) - 1) // 2
    copies = [
        pltpu.make_async_copy(source, target, sems.at[i])
        for i, (source, target) in enumerate(zip(refs[:half], refs[half:-1]))
    ]
    for copy in copies:
        copy.start()
    for copy in copies:
        copy.wait()


def hand_over(*results):
    vmem = pl.BlockSpec(memory_space=pltpu.VMEM)
    hbm = pl.BlockSpec(memory_space=pl.ANY)
    return pl.pallas_call(
        hand_over_kernel,
        out_shape=tuple(jax.ShapeDtypeStruct(r.shape, r.dtype) for r in results),
        in_specs=[vmem] * len(results),
        out_specs=(hbm,) * len(results),
        scratch_shapes=[pltpu.SemaphoreType.DMA((len(results),))],
        compiler_params=pltpu.CompilerParams(vmem_limit_bytes=1024 * 1024),
    )(*results)


def gathered_sums(activations, gradients, act_history, grad_history, owner_rank):
    my_rank = lax.axis_index("tensor")
    held = jnp.where(owner_rank[None, :] == my_rank, act_history[0], jnp.float32(0.0))
    current = lax.psum(held, "tensor")
    act_scale = QUANT_LIMIT / jnp.maximum(jnp.max(current, axis=0), SCALE_FLOOR)
    grad_scale = QUANT_LIMIT / jnp.maximum(jnp.max(grad_history, axis=0), SCALE_FLOOR)
    gathered_rows = lax.all_gather(quantize(activations, act_scale), "tensor", axis=0, tiled=True)
    summed = lax.psum_scatter(
        lax.dot_general(
            gathered_rows, quantize(gradients, grad_scale), (((0,), (0,)), ((), ())),
            preferred_element_type=jnp.float32,
        ),
        "dp", scatter_dimension=0, tiled=True,
    )
    act_peak = lax.pmax(jnp.max(jnp.abs(activations), axis=0).astype(jnp.float32), ("dp", "tensor"))
    grad_peak = lax.pmax(jnp.max(jnp.abs(gradients), axis=0).astype(jnp.float32), "dp")
    return summed, current, act_peak[None, :], grad_peak[None, :]


def body(activations, gradients, act_history, grad_history, owner_rank, history_slot):
    dp = lax.axis_size("dp")
    model_width = act_history.shape[2]
    column_total = gradients.shape[1]
    row_count = model_width // dp
    fits = dp == CORES * ROWS_Y * DEPTH
    fits = fits and (row_count * CORES) % LANES == 0 and row_count % (PIECES * 2 * SUBLANES) == 0
    fits = fits and model_width % (CORES * ROWS_Y * LANES) == 0 and activations.shape[0] % (TAIL_CUTS * TURN) == 0
    fits = fits and column_total % SUBLANES == 0
    if fits:
        return hand_over(*fused_outputs(
            activations, gradients, act_history, grad_history, owner_rank, history_slot
        ))
    act_slots = history_slot[:model_width]
    grad_slots = lax.dynamic_slice_in_dim(
        history_slot, model_width + lax.axis_index("tensor") * column_total, column_total, 0
    )
    summed, current, act_peak, grad_peak = gathered_sums(
        activations, gradients, act_history, grad_history, owner_rank
    )
    act_scale = QUANT_LIMIT / jnp.maximum(jnp.max(current, axis=0), SCALE_FLOOR)
    grad_scale = QUANT_LIMIT / jnp.maximum(jnp.max(grad_history, axis=0), SCALE_FLOOR)
    grad_factor = 1.0 / math.sqrt(gradients.shape[0] * dp)
    row_base = lax.axis_index("dp") * row_count
    row_scale = lax.dynamic_slice_in_dim(act_scale, row_base, row_count, 0)
    weight_grad = summed / (row_scale[:, None] * grad_scale[None, :]) * grad_factor
    act_history_out = place_peaks(current, act_peak[0], act_slots)[None]
    grad_history_out = place_peaks(grad_history, grad_peak[0], grad_slots)
    return (weight_grad, act_history_out, grad_history_out)


def solution(mesh):
    placed = (
        P(("dp", "tensor"), None),
        P("dp", "tensor"),
        P("tensor", None, None),
        P(None, "tensor"),
        P(),
        P(),
    )
    return jax.shard_map(
        body,
        mesh=mesh,
        in_specs=placed,
        out_specs=(P("dp", "tensor"), P("tensor", None, None), P(None, "tensor")),
        check_vma=False,
    )
```
